1024 devices in a mesh: gx: 4 (over x), gy: 16 (over y, core), gz: 16 (over z).
Axes of the slice: x: 4, y: 8, z: 16, core: 2. Of those that a mesh axis runs over, the one named last changes fastest.
Arguments:
- right_side: float32 [48, 256, 2048], P('gx', 'gy', 'gz'), may hold values from -8 to 8
- coefficient: float32 [48, 256, 2048], P('gx', 'gy', 'gz'), may hold values from 0.02 to 1
Outputs:
- solution: float32 [48, 256, 2048], P('gx', 'gy', 'gz')
- residual: float32 [48, 256, 2048], P('gx', 'gy', 'gz')
- precond: float32 [48, 256, 2048], P('gx', 'gy', 'gz')
- image: float32 [48, 256, 2048], P('gx', 'gy', 'gz')
The draws below stay inside these ranges and needn't reach their ends.
All inputs are finite; a program needn't handle non-finite values.
Results may differ from the reference program's by a relative error of at most 0.00021.
Values sent between devices are 32-bit elements; how exact they have to be, the bound alone decides.
A program may use at most 32 MiB of HBM per device.

```python
import math
import jax
import jax.numpy as jnp

SWEEPS = 4
ITERS = 1
NX = 48
NY = 256
NZ = 2048


def block_levels(own_key, shape, shards, smallest, largest):
    loudness, own = 1.0, jax.random.fold_in(own_key, 6)
    for position, parts in shards:
        steps = jnp.exp(jax.random.uniform(jax.random.fold_in(own, position), (parts,), jnp.float32, smallest / len(shards), largest / len(shards)))
        loudness = loudness * jnp.repeat(steps, shape[position] // parts).reshape([-1 if axis == position else 1 for axis in range(len(shape))])
    return loudness


def noise(own_key, shape, scale, reach, pieces=(), kind=jnp.bfloat16):
    values = jax.random.normal(own_key, shape, jnp.float32) * scale
    if len(pieces) > 0:
        values = block_levels(own_key, shape, pieces, -0.22, 0.18) * values
    return jnp.clip(values, min=-reach, max=reach).astype(kind)


def setup_inputs(seed: int = 0) -> dict:
    arg_keys = jax.random.split(jax.random.key(seed), 3)
    return {
        "right_side": noise(arg_keys[0], (NX, NY, NZ), 1.0, 8.0, ((0, 4), (1, 16), (2, 16)), jnp.float32),
        "coefficient": jnp.clip(jnp.exp(math.log(1.0) - 3.912023 * jax.random.uniform(arg_keys[1], (NX, NY, NZ), jnp.float32) ** block_levels(arg_keys[1], (NX, NY, NZ), ((0, 4), (1, 16), (2, 16)), -0.2, 0.2)), 0.02, 1.0),
    }


relaxation = 0.6


def block_sum(padded):
    summed = padded[:-2] + padded[1:-1] + padded[2:]
    summed = summed[:, :-2] + summed[:, 1:-1] + summed[:, 2:]
    return summed[:, :, :-2] + summed[:, :, 1:-1] + summed[:, :, 2:]


def operate(values, reaction):
    return (27.0 + reaction) * values - block_sum(jnp.pad(values, 1))


def restrict(values):
    extent = values.shape
    grouped = values.reshape(extent[0] // 2, 2, extent[1] // 2, 2, extent[2] // 2, 2)
    return 0.5 * grouped.sum(axis=(1, 3, 5))


def prolong(values):
    return jnp.repeat(jnp.repeat(jnp.repeat(values, 2, axis=0), 2, axis=1), 2, axis=2)


def coarsest(source, reaction):
    correction = relaxation * source / (26.0 + reaction)
    for sweep in range(SWEEPS - 1):
        correction = correction + relaxation * (source - operate(correction, reaction)) / (26.0 + reaction)
    return correction


def multigrid(source, reactions, level_index):
    if level_index == 2:
        return coarsest(source, reactions[2])
    reaction = reactions[level_index]
    correction = relaxation * source / (26.0 + reaction)
    remainder = source - operate(correction, reaction)
    correction = correction + prolong(multigrid(restrict(remainder), reactions, level_index + 1))
    return correction + relaxation * (source - operate(correction, reaction)) / (26.0 + reaction)


def reference(right_side, coefficient):
    middle = restrict(coefficient)
    reactions = (coefficient, middle, restrict(middle))
    solution = jnp.zeros_like(right_side)
    residual = right_side
    precond = multigrid(residual, reactions, 0)
    image = operate(precond, coefficient)
    direction = precond
    dir_image = image
    dir_precond = precond
    dir_twice = image
    gamma_prev = jnp.float32(1.0)
    alpha_prev = jnp.float32(1.0)
    for step in range(ITERS):
        gamma_now = jnp.sum(residual * precond)
        delta_now = jnp.sum(image * precond)
        precond_image = multigrid(image, reactions, 0)
        image_twice = operate(precond_image, coefficient)
        if step == 0:
            alpha_now = gamma_now / delta_now
            direction = precond
            dir_image = image
            dir_precond = precond_image
            dir_twice = image_twice
        else:
            beta_now = gamma_now / gamma_prev
            alpha_now = gamma_now / (delta_now - beta_now * gamma_now / alpha_prev)
            dir_twice = image_twice + beta_now * dir_twice
            dir_precond = precond_image + beta_now * dir_precond
            dir_image = image + beta_now * dir_image
            direction = precond + beta_now * direction
        solution = solution + alpha_now * direction
        residual = residual - alpha_now * dir_image
        precond = precond - alpha_now * dir_precond
        image = image - alpha_now * dir_twice
        gamma_prev = gamma_now
        alpha_prev = alpha_now
    return (solution, residual, precond, image)
```

```python
import functools

import jax
import jax.numpy as jnp
from jax import lax
from jax.experimental import pallas as pl
from jax.experimental.pallas import tpu as pltpu
from jax.sharding import PartitionSpec as P

MESH = pl.DeviceIdType.MESH
F32 = jnp.float32
BF16 = jnp.bfloat16

BX, BY, BZ = 12, 16, 128
CX, CY, CZ = 3, 4, 32
HX = 5
LX = BX + 2 * HX
LY = 32
FINE = [
    (dx, dy, dz)
    for dx in (-1, 0, 1)
    for dy in (-1, 0, 1)
    for dz in (-1, 0, 1)
    if (dx, dy, dz) != (0, 0, 0)
]
DEEP = [
    (dx, dy, dz)
    for dx in (-2, -1, 0, 1, 2)
    for dy in (-1, 0, 1)
    for dz in (-1, 0, 1)
    if (dx, dy, dz) != (0, 0, 0)
]


def iota(shape, axis):
    return lax.broadcasted_iota(jnp.int32, shape, axis)


def split(values):
    high = values.astype(BF16)
    rest = values - high.astype(F32)
    middle = rest.astype(BF16)
    low = (rest - middle.astype(F32)).astype(BF16)
    return high, middle, low


def select_dot(values, table):
    high, middle, low = split(values)
    dot = functools.partial(jnp.dot, preferred_element_type=F32)
    return dot(low, table) + dot(middle, table) + dot(high, table)


def ones_where(condition):
    return jnp.where(condition, 1.0, 0.0).astype(BF16)


def wrapped(lane, size):
    return jnp.where(lane < size * 3 // 4, lane, lane - size)


def around(plane):
    rows, lanes = plane.shape[-2:]
    axis = plane.ndim - 2
    plane = plane + pltpu.roll(plane, 1, axis) + pltpu.roll(plane, rows - 1, axis)
    return plane + pltpu.roll(plane, 1, axis + 1) + pltpu.roll(plane, lanes - 1, axis + 1)


def loop(count, unroll, body):
    def step(i, carry):
        body(i)
        return carry

    lax.fori_loop(0, count, step, 0, unroll=unroll)


def kernel(
    sizes,
    g_hbm, c_hbm,
    p_out, image_out, mw_out, nw_out, sums_out,
    own, ext, packed, halo, coarse_own, coarse_ext,
    wide, inv0, e0, rest0, inv1, g1, e1, inv2, coarse,
    t_fine, t_mid, p_mid, p_fine,
    m_pack, m_unpack, m_r0, m_r1, m_p1, m_p0,
    load_sem, fine_send, fine_recv, deep_send, deep_recv,
):
    nx, ny, nz = sizes
    gx, gy, gz = lax.axis_index("gx"), lax.axis_index("gy"), lax.axis_index("gz")

    def exists(d):
        checks = []
        for delta, at, count in zip(d, (gx, gy, gz), sizes):
            if delta < 0:
                checks.append(at >= -delta)
            if delta > 0:
                checks.append(at < count - delta)
        return functools.reduce(jnp.logical_and, checks)

    def device(d):
        return (gx + d[0], gy + d[1], gz + d[2])

    loads = [
        pltpu.make_async_copy(g_hbm, own.at[0], load_sem.at[0]),
        pltpu.make_async_copy(c_hbm, own.at[1], load_sem.at[1]),
    ]
    for load in loads:
        load.start()

    ext[...] = jnp.zeros_like(ext)
    halo[...] = jnp.zeros_like(halo)
    coarse_ext[...] = jnp.zeros_like(coarse_ext)

    barrier = pltpu.get_barrier_semaphore()
    for d in DEEP:
        @pl.when(exists(d))
        def _(d=d):
            pl.semaphore_signal(barrier, inc=1, device_id=device(d), device_id_type=MESH)

    row, col = iota((BZ, 2 * BZ), 0), iota((BZ, 2 * BZ), 1)
    m_pack[...] = ones_where(row == jnp.where(col < BZ, col % 8, 120 + col % 8))
    row, col = iota((2 * BZ, BZ), 0), iota((2 * BZ, BZ), 1)
    m_unpack[...] = ones_where(col == jnp.where(row < BZ, 120 + row % 8, row % 8))
    m_r0[...] = ones_where(col == (jnp.where(row < 192, row, row - 256) >> 1) % 128)
    row, col = iota((BZ, BZ), 0), iota((BZ, BZ), 1)
    m_r1[...] = ones_where(jnp.logical_and(row < 64, (row >> 1) == col % 32))
    m_p1[...] = ones_where(row == (wrapped(col, 128) >> 1) % 128)
    row, col = iota((BZ, 2 * BZ), 0), iota((BZ, 2 * BZ), 1)
    m_p0[...] = ones_where(row == (wrapped(col, 256) >> 1) % 128)

    def pack(field):
        values = own[field].reshape(BX * BY, BZ)
        spread = select_dot(values, m_pack[...]).reshape(BX, BY, 2 * BZ)
        lane, row = iota((BX, BY, 2 * BZ), 2), iota((BX, BY, 2 * BZ), 1)
        spread = jnp.where((lane % 128) // 8 == row, spread, 0.0)
        flat = jnp.sum(spread, axis=1, keepdims=True)
        packed[0, field] = flat[:, :, :BZ]
        packed[1, field] = flat[:, :, BZ:]

    def fine_copies(first, count):
        fields = pl.ds(first, count)
        for n, (dx, dy, dz) in enumerate(FINE):
            source = {-1: pl.ds(0, HX), 0: pl.ds(0, BX), 1: pl.ds(BX - HX, HX)}[dx]
            target = {-1: pl.ds(HX + BX, HX), 0: pl.ds(HX, BX), 1: pl.ds(0, HX)}[dx]
            if dz == 0:
                rows = {-1: pl.ds(0, 8), 0: pl.ds(0, 16), 1: pl.ds(8, 8)}[dy]
                to = {-1: pl.ds(24, 8), 0: pl.ds(8, 16), 1: pl.ds(0, 8)}[dy]
                src, dst = own.at[fields, source, rows], ext.at[fields, target, to]
            else:
                src = packed.at[(dz + 1) // 2, fields, source]
                dst = halo.at[(1 - dz) // 2, fields, 1 - dy, target]
            yield n, (dx, dy, dz), pltpu.make_async_remote_copy(
                src_ref=src, dst_ref=dst, send_sem=fine_send.at[n], recv_sem=fine_recv.at[n],
                device_id=device((dx, dy, dz)), device_id_type=MESH,
            )

    def deep_copies(part):
        fields = pl.ds(0, 2) if part == 0 else pl.ds(2, 1)
        for n, (dx, dy, dz) in enumerate(DEEP):
            yield n, (dx, dy, dz), pltpu.make_async_remote_copy(
                src_ref=coarse_own.at[fields],
                dst_ref=coarse_ext.at[fields, 1 - dy, 1 - dz, pl.ds(CX * gx, CX)],
                send_sem=deep_send.at[part, n], recv_sem=deep_recv.at[part, n],
                device_id=device((dx, dy, dz)), device_id_type=MESH,
            )

    def start(copies):
        for n, d, copy in copies:
            @pl.when(exists(d))
            def _(copy=copy):
                copy.start()

    def finish(copies):
        copies = list(copies)
        for n, d, copy in copies:
            @pl.when(exists(tuple(-s for s in d)))
            def _(copy=copy):
                copy.wait_recv()
        for n, d, copy in copies:
            @pl.when(exists(d))
            def _(copy=copy):
                copy.wait_send()

    def widen(field):
        ext[field, HX : HX + BX, 8:24] = own[field]
        lane, row = iota((LY, BZ), 1), iota((LY, BZ), 0)
        fits = (lane // 8) == (row + 8) % 16
        sides = []
        for side in (0, 1):
            rows = jnp.concatenate(
                [
                    jnp.broadcast_to(halo[side, field, 0], (LX, 8, BZ)),
                    jnp.broadcast_to(halo[side, field, 1], (LX, 16, BZ)),
                    jnp.broadcast_to(halo[side, field, 2], (LX, 8, BZ)),
                ],
                axis=1,
            )
            sides.append(jnp.where(fits[None], rows, 0.0).reshape(LX * LY, BZ))
        outer = select_dot(sides[0], m_unpack[:BZ]) + select_dot(sides[1], m_unpack[BZ:])
        wide[:, :, :BZ] = ext[field]
        wide[:, :, BZ:] = outer.reshape(LX, LY, BZ)

    def restrict_fine():
        t_fine[...] = select_dot(rest0[...].reshape(10 * LY, 2 * BZ), m_r0[...]).reshape(10, LY, BZ)
        return 0.5 * (t_fine[:, pl.ds(0, 16, stride=2)] + t_fine[:, pl.ds(1, 16, stride=2)])

    def restrict_mid(values):
        pairs = values.reshape(CX, 2, 16, BZ)
        pairs = pairs[:, 0] + pairs[:, 1]
        t_mid[...] = select_dot(pairs.reshape(CX * 16, BZ), m_r1[...]).reshape(CX, 16, BZ)
        cells = 0.5 * (t_mid[:, pl.ds(0, 8, stride=2)] + t_mid[:, pl.ds(1, 8, stride=2)])
        lane, row = iota((8, BZ), 1), iota((8, BZ), 0)
        return jnp.sum(jnp.where((lane // 32 == row - 2)[None], cells, 0.0), axis=1, keepdims=True)

    def put_coarse(field, cells):
        coarse_own[field] = cells
        coarse_ext[field, 1, 1, pl.ds(CX * gx, CX)] = cells

    def coarse_field(field):
        shape = (CX * nx, 16, BZ)
        lane, row = iota((16, BZ), 1), iota((16, BZ), 0)
        y = jnp.where(row < 10, row - 2, row - 18)
        slot, group = (y + 4) // 4, (row + 2) % 4
        total = None
        for dz in (-1, 0, 1):
            rows = jnp.zeros(shape, F32)
            for dy in (-1, 0, 1):
                fits = jnp.logical_and(slot == dy + 1, lane // 32 == group)
                taken = jnp.broadcast_to(coarse_ext[field, dy + 1, dz + 1], shape)
                rows = jnp.where(fits[None], taken, rows)
            rows = rows + pltpu.roll(rows, 32, 2)
            rows = rows + pltpu.roll(rows, 64, 2)
            rows = jnp.where((lane // 32 == dz % 4)[None], rows, 0.0)
            total = rows if total is None else total + rows
        return total

    def inside(layer, low, size, first, shape, x_first, y_of, z_of):
        pass

    def masked_inverse(values, x, y, z, scale):
        ok = jnp.logical_and(y >= 0, y < scale * CY * ny)
        ok = jnp.logical_and(ok, jnp.logical_and(z >= 0, z < scale * CZ * nz))
        if x is not None:
            ok = jnp.logical_and(ok, jnp.logical_and(x >= 0, x < scale * CX * nx))
        return jnp.where(ok, 0.6 / (26.0 + values), 0.0)

    def coefficients():
        lane, row = iota((LY, 2 * BZ), 1), iota((LY, 2 * BZ), 0)
        y, z = BY * gy + row - 8, BZ * gz + wrapped(lane, 256)

        def body(i):
            inv0[i] = masked_inverse(wide[i], BX * gx + i - HX, y, z, 4)

        loop(LX, 2, body)

        def pairs(j):
            rest0[j] = wide[2 * j + 1] + wide[2 * j + 2]

        loop(10, 2, pairs)
        c1 = restrict_fine()
        put_coarse(1, restrict_mid(c1[2:8]))
        shape = (10, 16, BZ)
        x = 2 * CX * gx + iota(shape, 0) - 2
        y = 2 * CY * gy + iota(shape, 1) - 4
        z = 2 * CZ * gz + wrapped(iota(shape, 2), 128)
        inv1[...] = masked_inverse(c1, x, y, z, 2)

    def down():
        def guess(i):
            e0[i] = inv0[i] * wide[i]

        loop(LX, 2, guess)

        def rest(j):
            i = 2 * j
            e_0, e_1, e_2, e_3 = e0[i], e0[i + 1], e0[i + 2], e0[i + 3]
            middle = e_1 + e_2
            total = around(e_0 + middle + (middle + e_3)) - middle
            rest0[j] = 0.4 * (wide[i + 1] + wide[i + 2]) + total

        loop(10, 2, rest)
        right = restrict_fine()
        g1[...] = right
        first = inv1[...] * right
        e1[...] = first
        total = first[1:7] + first[2:8] + first[3:9]
        remainder = 0.4 * right[2:8] + around(total) - first[2:8]
        return restrict_mid(remainder)

    def solve_coarsest(right):
        inverse = inv2[...]
        edge = jnp.zeros((1, 16, BZ), F32)
        e = inverse * right
        for _ in range(3):
            padded = jnp.concatenate([edge, e, edge], axis=0)
            total = around(padded[:-2] + padded[1:-1] + padded[2:])
            e = 0.4 * e + inverse * (right + total - e)
        coarse[pl.ds(1, CX * nx)] = e

    def up(keep):
        near = coarse[pl.ds(CX * gx, CX + 2)][:, :8]
        p_mid[:, pl.ds(0, 8, stride=2)] = near
        p_mid[:, pl.ds(1, 8, stride=2)] = near
        rise = select_dot(p_mid[...].reshape(5 * 16, BZ), m_p1[...]).reshape(5, 1, 16, BZ)
        rise = jnp.broadcast_to(rise, (5, 2, 16, BZ)).reshape(10, 16, BZ)
        e = e1[...] + rise
        total = around(e[0:8] + e[1:9] + e[2:10])
        e = 0.4 * e[1:9] + inv1[1:9] * (g1[1:9] + total - e[1:9])
        p_fine[:, pl.ds(0, 16, stride=2)] = e
        p_fine[:, pl.ds(1, 16, stride=2)] = e
        rest0[pl.ds(0, 8)] = select_dot(p_fine[...].reshape(8 * LY, BZ), m_p0[...]).reshape(8, LY, 2 * BZ)

        def add(j):
            i = 2 * j + 3
            e0[i] = e0[i] + rest0[j]
            e0[i + 1] = e0[i + 1] + rest0[j]

        loop(8, 2, add)

        def smooth(k):
            i = k + 4
            e = e0[i]
            total = around(e0[i - 1] + e + e0[i + 1])
            keep(i, 0.4 * e + inv0[i] * (wide[i] + total - e))

        loop(14, 2, smooth)

    def operate(keep):
        def body(x):
            i = x + HX
            value = wide[i]
            total = around(wide[i - 1] + value + wide[i + 1])
            value, total = value[8:24, :BZ], total[8:24, :BZ]
            keep(x, value, (27.0 + own[1, x]) * value - total)

        loop(BX, 2, body)

    def keep_wide(i, plane):
        wide[i] = plane

    for load in loads:
        load.wait()
    pack(0)
    pack(1)
    count = jnp.int32(0)
    for d in DEEP:
        count = count + exists(d).astype(jnp.int32)
    pl.semaphore_wait(barrier, count)

    start(fine_copies(0, 2))
    finish(fine_copies(0, 2))
    widen(1)
    coefficients()
    widen(0)
    put_coarse(0, down())
    start(deep_copies(0))
    finish(deep_copies(0))
    shape = (CX * nx, 16, BZ)
    row = iota(shape, 1)
    y = CY * gy + jnp.where(row < 10, row - 2, row - 18)
    z = CZ * gz + wrapped(iota(shape, 2), 128)
    inv2[...] = masked_inverse(coarse_field(1), None, y, z, 1)
    edge = jnp.zeros((16, BZ), F32)
    coarse[0] = edge
    coarse[CX * nx + 1] = edge
    solve_coarsest(coarse_field(0))
    up(keep_wide)

    sums_out[...] = jnp.zeros_like(sums_out)

    def first_image(x, value, image):
        p_out[x] = value
        image_out[x] = image
        own[2, x] = image
        sums_out[0] += own[0, x] * value
        sums_out[1] += image * value

    operate(first_image)

    pack(2)
    start(fine_copies(2, 1))
    finish(fine_copies(2, 1))
    widen(2)
    put_coarse(2, down())
    start(deep_copies(1))
    finish(deep_copies(1))
    solve_coarsest(coarse_field(2))
    up(keep_wide)

    def second_image(x, value, image):
        mw_out[x] = value
        nw_out[x] = image

    operate(second_image)


def call(sizes, right_side, coefficient):
    nx = sizes[0]
    block = jax.ShapeDtypeStruct((BX, BY, BZ), F32)
    any_spec = pl.BlockSpec(memory_space=pl.ANY)
    vmem_spec = pl.BlockSpec(memory_space=pltpu.VMEM)
    vmem = pltpu.VMEM
    return pl.pallas_call(
        functools.partial(kernel, sizes),
        out_shape=[block] * 4 + [jax.ShapeDtypeStruct((2, BY, BZ), F32)],
        in_specs=[any_spec] * 2,
        out_specs=[vmem_spec] * 5,
        scratch_shapes=[
            vmem((3, BX, BY, BZ), F32),
            vmem((3, LX, LY, BZ), F32),
            vmem((2, 3, BX, 1, BZ), F32),
            vmem((2, 3, 3, LX, 1, BZ), F32),
            vmem((3, CX, 1, BZ), F32),
            vmem((3, 3, 3, CX * nx, 1, BZ), F32),
            vmem((LX, LY, 2 * BZ), F32),
            vmem((LX, LY, 2 * BZ), F32),
            vmem((LX, LY, 2 * BZ), F32),
            vmem((10, LY, 2 * BZ), F32),
            vmem((10, 16, BZ), F32),
            vmem((10, 16, BZ), F32),
            vmem((10, 16, BZ), F32),
            vmem((CX * nx, 16, BZ), F32),
            vmem((CX * nx + 2, 16, BZ), F32),
            vmem((10, LY, BZ), F32),
            vmem((CX, 16, BZ), F32),
            vmem((5, 16, BZ), F32),
            vmem((8, LY, BZ), F32),
            vmem((BZ, 2 * BZ), BF16),
            vmem((2 * BZ, BZ), BF16),
            vmem((2 * BZ, BZ), BF16),
            vmem((BZ, BZ), BF16),
            vmem((BZ, BZ), BF16),
            vmem((BZ, 2 * BZ), BF16),
            pltpu.SemaphoreType.DMA((2,)),
            pltpu.SemaphoreType.DMA((len(FINE),)),
            pltpu.SemaphoreType.DMA((len(FINE),)),
            pltpu.SemaphoreType.DMA((2, len(DEEP))),
            pltpu.SemaphoreType.DMA((2, len(DEEP))),
        ],
        compiler_params=pltpu.CompilerParams(collective_id=0, has_side_effects=True),
    )(right_side, coefficient)


def solution(mesh):
    sizes = tuple(mesh.shape[axis] for axis in ("gx", "gy", "gz"))

    def shards(right_side, coefficient):
        precond, image, mw, nw, sums = call(sizes, right_side, coefficient)
        totals = lax.psum(jnp.sum(sums, axis=(1, 2)), ("gx", "gy", "gz"))
        alpha = totals[0] / totals[1]
        return (
            alpha * precond,
            right_side - alpha * image,
            precond - alpha * mw,
            image - alpha * nw,
        )

    spec = P("gx", "gy", "gz")
    return jax.shard_map(
        shards, mesh=mesh, in_specs=(spec, spec), out_specs=(spec,) * 4, check_vma=False
    )
```

```python
import functools

import jax
import jax.numpy as jnp
from jax import lax
from jax.experimental import pallas as pl
from jax.experimental.pallas import tpu as pltpu
from jax.sharding import PartitionSpec as P

MESH = pl.DeviceIdType.MESH
F32 = jnp.float32
BF16 = jnp.bfloat16

BX, BY, BZ = 12, 16, 128
CX, CY, CZ = 3, 4, 32
HX = 5
LX = BX + 2 * HX
LY = 32
FINE = [
    (dx, dy, dz)
    for dx in (-1, 0, 1)
    for dy in (-1, 0, 1)
    for dz in (-1, 0, 1)
    if (dx, dy, dz) != (0, 0, 0)
]
DEEP = [
    (dx, dy, dz)
    for dx in (-2, -1, 0, 1, 2)
    for dy in (-1, 0, 1)
    for dz in (-1, 0, 1)
    if (dx, dy, dz) != (0, 0, 0)
]


def iota(shape, axis):
    return lax.broadcasted_iota(jnp.int32, shape, axis)


def split(values):
    high = values.astype(BF16)
    rest = values - high.astype(F32)
    middle = rest.astype(BF16)
    low = (rest - middle.astype(F32)).astype(BF16)
    return high, middle, low


def select_dot(values, table):
    high, middle, low = split(values)
    dot = functools.partial(jnp.dot, preferred_element_type=F32)
    return dot(low, table) + dot(middle, table) + dot(high, table)


def ones_where(condition):
    return jnp.where(condition, 1.0, 0.0).astype(BF16)


def wrapped(lane, size):
    return jnp.where(lane < size * 3 // 4, lane, lane - size)


def around(plane):
    rows, lanes = plane.shape[-2:]
    axis = plane.ndim - 2
    plane = plane + pltpu.roll(plane, 1, axis) + pltpu.roll(plane, rows - 1, axis)
    return plane + pltpu.roll(plane, 1, axis + 1) + pltpu.roll(plane, lanes - 1, axis + 1)


def loop(count, unroll, body):
    def step(i, carry):
        body(i)
        return carry

    lax.fori_loop(0, count, step, 0, unroll=unroll)


def kernel(
    sizes,
    g_hbm, c_hbm,
    p_out, image_out, mw_out, nw_out, alpha_out,
    own, ext, packed, halo, coarse_own, coarse_ext,
    wide, inv0, e0, rest0, inv1, g1, e1, inv2, coarse,
    t_fine, t_mid, p_mid, p_fine,
    m_pack, m_unpack, m_r0, m_r1, m_p1, m_p0,
    sums, line_own, line_0, line_1, line_2,
    load_sem, fine_send, fine_recv, deep_send, deep_recv, line_send, line_recv,
):
    nx, ny, nz = sizes
    gx, gy, gz = lax.axis_index("gx"), lax.axis_index("gy"), lax.axis_index("gz")

    def exists(d):
        checks = []
        for delta, at, count in zip(d, (gx, gy, gz), sizes):
            if delta < 0:
                checks.append(at >= -delta)
            if delta > 0:
                checks.append(at < count - delta)
        return functools.reduce(jnp.logical_and, checks)

    def device(d):
        return (gx + d[0], gy + d[1], gz + d[2])

    def along(axis, k):
        at = [gx, gy, gz]
        at[axis] = lax.rem(at[axis] + k, sizes[axis])
        return tuple(at)

    loads = [
        pltpu.make_async_copy(g_hbm, own.at[0], load_sem.at[0]),
        pltpu.make_async_copy(c_hbm, own.at[1], load_sem.at[1]),
    ]
    for load in loads:
        load.start()

    ext[...] = jnp.zeros_like(ext)
    halo[...] = jnp.zeros_like(halo)
    coarse_ext[...] = jnp.zeros_like(coarse_ext)

    barrier = pltpu.get_barrier_semaphore()
    count = jnp.int32(sum(sizes) - 3)
    for d in DEEP:
        if sum(s != 0 for s in d) == 1:
            continue
        count = count + exists(d).astype(jnp.int32)

        @pl.when(exists(d))
        def _(d=d):
            pl.semaphore_signal(barrier, inc=1, device_id=device(d), device_id_type=MESH)

    for axis in range(3):
        for k in range(1, sizes[axis]):
            pl.semaphore_signal(barrier, inc=1, device_id=along(axis, k), device_id_type=MESH)

    row, col = iota((BZ, 2 * BZ), 0), iota((BZ, 2 * BZ), 1)
    m_pack[...] = ones_where(row == jnp.where(col < BZ, col % 8, 120 + col % 8))
    row, col = iota((2 * BZ, BZ), 0), iota((2 * BZ, BZ), 1)
    m_unpack[...] = ones_where(col == jnp.where(row < BZ, 120 + row % 8, row % 8))
    m_r0[...] = ones_where(col == (jnp.where(row < 192, row, row - 256) >> 1) % 128)
    row, col = iota((BZ, BZ), 0), iota((BZ, BZ), 1)
    m_r1[...] = ones_where(jnp.logical_and(row < 64, (row >> 1) == col % 32))
    m_p1[...] = ones_where(row == (wrapped(col, 128) >> 1) % 128)
    row, col = iota((BZ, 2 * BZ), 0), iota((BZ, 2 * BZ), 1)
    m_p0[...] = ones_where(row == (wrapped(col, 256) >> 1) % 128)

    def pack(field):
        values = own[field].reshape(BX * BY, BZ)
        spread = select_dot(values, m_pack[...]).reshape(BX, BY, 2 * BZ)
        lane, row = iota((BX, BY, 2 * BZ), 2), iota((BX, BY, 2 * BZ), 1)
        spread = jnp.where((lane % 128) // 8 == row, spread, 0.0)
        flat = jnp.sum(spread, axis=1, keepdims=True)
        packed[0, field] = flat[:, :, :BZ]
        packed[1, field] = flat[:, :, BZ:]

    def fine_copies(first, count):
        fields = pl.ds(first, count)
        for n, (dx, dy, dz) in enumerate(FINE):
            source = {-1: pl.ds(0, HX), 0: pl.ds(0, BX), 1: pl.ds(BX - HX, HX)}[dx]
            target = {-1: pl.ds(HX + BX, HX), 0: pl.ds(HX, BX), 1: pl.ds(0, HX)}[dx]
            if dz == 0:
                rows = {-1: pl.ds(0, 8), 0: pl.ds(0, 16), 1: pl.ds(8, 8)}[dy]
                to = {-1: pl.ds(24, 8), 0: pl.ds(8, 16), 1: pl.ds(0, 8)}[dy]
                src, dst = own.at[fields, source, rows], ext.at[fields, target, to]
            else:
                src = packed.at[(dz + 1) // 2, fields, source]
                dst = halo.at[(1 - dz) // 2, fields, 1 - dy, target]
            yield n, (dx, dy, dz), pltpu.make_async_remote_copy(
                src_ref=src, dst_ref=dst, send_sem=fine_send.at[n], recv_sem=fine_recv.at[n],
                device_id=device((dx, dy, dz)), device_id_type=MESH,
            )

    def deep_copies(part):
        fields = pl.ds(0, 2) if part == 0 else pl.ds(2, 1)
        for n, (dx, dy, dz) in enumerate(DEEP):
            yield n, (dx, dy, dz), pltpu.make_async_remote_copy(
                src_ref=coarse_own.at[fields],
                dst_ref=coarse_ext.at[fields, 1 - dy, 1 - dz, pl.ds(CX * gx, CX)],
                send_sem=deep_send.at[part, n], recv_sem=deep_recv.at[part, n],
                device_id=device((dx, dy, dz)), device_id_type=MESH,
            )

    def start(copies):
        for n, d, copy in copies:
            @pl.when(exists(d))
            def _(copy=copy):
                copy.start()

    def finish(copies):
        copies = list(copies)
        for n, d, copy in copies:
            @pl.when(exists(tuple(-s for s in d)))
            def _(copy=copy):
                copy.wait_recv()
        for n, d, copy in copies:
            @pl.when(exists(d))
            def _(copy=copy):
                copy.wait_send()

    lines = (line_0, line_1, line_2)

    def line_copies(axis):
        me = (gx, gy, gz)[axis]
        for k in range(1, sizes[axis]):
            yield pltpu.make_async_remote_copy(
                src_ref=line_own.at[axis], dst_ref=lines[axis].at[me],
                send_sem=line_send.at[axis, k], recv_sem=line_recv.at[axis, k],
                device_id=along(axis, k), device_id_type=MESH,
            )

    def line_start(axis, row):
        line_own[axis] = row
        lines[axis][(gx, gy, gz)[axis]] = row
        for copy in line_copies(axis):
            copy.start()

    def line_finish(axis):
        copies = list(line_copies(axis))
        for copy in copies:
            copy.wait_recv()
        for copy in copies:
            copy.wait_send()
        return jnp.sum(lines[axis][...], axis=0)

    def widen(field):
        ext[field, HX : HX + BX, 8:24] = own[field]
        lane, row = iota((LY, BZ), 1), iota((LY, BZ), 0)
        fits = (lane // 8) == (row + 8) % 16
        sides = []
        for side in (0, 1):
            rows = jnp.concatenate(
                [
                    jnp.broadcast_to(halo[side, field, 0], (LX, 8, BZ)),
                    jnp.broadcast_to(halo[side, field, 1], (LX, 16, BZ)),
                    jnp.broadcast_to(halo[side, field, 2], (LX, 8, BZ)),
                ],
                axis=1,
            )
            sides.append(jnp.where(fits[None], rows, 0.0).reshape(LX * LY, BZ))
        outer = select_dot(sides[0], m_unpack[:BZ]) + select_dot(sides[1], m_unpack[BZ:])
        wide[:, :, :BZ] = ext[field]
        wide[:, :, BZ:] = outer.reshape(LX, LY, BZ)

    def restrict_fine():
        t_fine[...] = select_dot(rest0[...].reshape(10 * LY, 2 * BZ), m_r0[...]).reshape(10, LY, BZ)
        return 0.5 * (t_fine[:, pl.ds(0, 16, stride=2)] + t_fine[:, pl.ds(1, 16, stride=2)])

    def restrict_mid(values):
        pairs = values.reshape(CX, 2, 16, BZ)
        pairs = pairs[:, 0] + pairs[:, 1]
        t_mid[...] = select_dot(pairs.reshape(CX * 16, BZ), m_r1[...]).reshape(CX, 16, BZ)
        cells = 0.5 * (t_mid[:, pl.ds(0, 8, stride=2)] + t_mid[:, pl.ds(1, 8, stride=2)])
        lane, row = iota((8, BZ), 1), iota((8, BZ), 0)
        return jnp.sum(jnp.where((lane // 32 == row - 2)[None], cells, 0.0), axis=1, keepdims=True)

    def put_coarse(field, cells):
        coarse_own[field] = cells
        coarse_ext[field, 1, 1, pl.ds(CX * gx, CX)] = cells

    def coarse_field(field):
        shape = (CX * nx, 16, BZ)
        lane, row = iota((16, BZ), 1), iota((16, BZ), 0)
        y = jnp.where(row < 10, row - 2, row - 18)
        slot, group = (y + 4) // 4, (row + 2) % 4
        total = None
        for dz in (-1, 0, 1):
            rows = jnp.zeros(shape, F32)
            for dy in (-1, 0, 1):
                fits = jnp.logical_and(slot == dy + 1, lane // 32 == group)
                taken = jnp.broadcast_to(coarse_ext[field, dy + 1, dz + 1], shape)
                rows = jnp.where(fits[None], taken, rows)
            rows = rows + pltpu.roll(rows, 32, 2)
            rows = rows + pltpu.roll(rows, 64, 2)
            rows = jnp.where((lane // 32 == dz % 4)[None], rows, 0.0)
            total = rows if total is None else total + rows
        return total

    def masked_inverse(values, x, y, z, scale):
        ok = jnp.logical_and(y >= 0, y < scale * CY * ny)
        ok = jnp.logical_and(ok, jnp.logical_and(z >= 0, z < scale * CZ * nz))
        if x is not None:
            ok = jnp.logical_and(ok, jnp.logical_and(x >= 0, x < scale * CX * nx))
        return jnp.where(ok, 0.6 / (26.0 + values), 0.0)

    def coefficients():
        lane, row = iota((LY, 2 * BZ), 1), iota((LY, 2 * BZ), 0)
        y, z = BY * gy + row - 8, BZ * gz + wrapped(lane, 256)

        def body(i):
            inv0[i] = masked_inverse(wide[i], BX * gx + i - HX, y, z, 4)

        loop(LX, 2, body)

        def pairs(j):
            rest0[j] = wide[2 * j + 1] + wide[2 * j + 2]

        loop(10, 2, pairs)
        c1 = restrict_fine()
        put_coarse(1, restrict_mid(c1[2:8]))
        shape = (10, 16, BZ)
        x = 2 * CX * gx + iota(shape, 0) - 2
        y = 2 * CY * gy + iota(shape, 1) - 4
        z = 2 * CZ * gz + wrapped(iota(shape, 2), 128)
        inv1[...] = masked_inverse(c1, x, y, z, 2)

    def down():
        def guess(i):
            e0[i] = inv0[i] * wide[i]

        loop(LX, 2, guess)

        def rest(j):
            i = 2 * j
            e_0, e_1, e_2, e_3 = e0[i], e0[i + 1], e0[i + 2], e0[i + 3]
            middle = e_1 + e_2
            total = around(e_0 + middle + (middle + e_3)) - middle
            rest0[j] = 0.4 * (wide[i + 1] + wide[i + 2]) + total

        loop(10, 2, rest)
        right = restrict_fine()
        g1[...] = right
        first = inv1[...] * right
        e1[...] = first
        total = first[1:7] + first[2:8] + first[3:9]
        remainder = 0.4 * right[2:8] + around(total) - first[2:8]
        return restrict_mid(remainder)

    def solve_coarsest(right):
        inverse = inv2[...]
        edge = jnp.zeros((1, 16, BZ), F32)
        e = inverse * right
        for _ in range(3):
            padded = jnp.concatenate([edge, e, edge], axis=0)
            total = around(padded[:-2] + padded[1:-1] + padded[2:])
            e = 0.4 * e + inverse * (right + total - e)
        coarse[pl.ds(1, CX * nx)] = e

    def up(keep):
        near = coarse[pl.ds(CX * gx, CX + 2)][:, :8]
        p_mid[:, pl.ds(0, 8, stride=2)] = near
        p_mid[:, pl.ds(1, 8, stride=2)] = near
        rise = select_dot(p_mid[...].reshape(5 * 16, BZ), m_p1[...]).reshape(5, 1, 16, BZ)
        rise = jnp.broadcast_to(rise, (5, 2, 16, BZ)).reshape(10, 16, BZ)
        e = e1[...] + rise
        total = around(e[0:8] + e[1:9] + e[2:10])
        e = 0.4 * e[1:9] + inv1[1:9] * (g1[1:9] + total - e[1:9])
        p_fine[:, pl.ds(0, 16, stride=2)] = e
        p_fine[:, pl.ds(1, 16, stride=2)] = e
        rest0[pl.ds(0, 8)] = select_dot(p_fine[...].reshape(8 * LY, BZ), m_p0[...]).reshape(8, LY, 2 * BZ)

        def add(j):
            i = 2 * j + 3
            e0[i] = e0[i] + rest0[j]
            e0[i + 1] = e0[i + 1] + rest0[j]

        loop(8, 2, add)

        def smooth(k):
            i = k + 4
            e = e0[i]
            total = around(e0[i - 1] + e + e0[i + 1])
            keep(i, 0.4 * e + inv0[i] * (wide[i] + total - e))

        loop(14, 2, smooth)

    def operate(keep):
        def body(x):
            i = x + HX
            value = wide[i]
            total = around(wide[i - 1] + value + wide[i + 1])
            value, total = value[8:24, :BZ], total[8:24, :BZ]
            keep(x, value, (27.0 + own[1, x]) * value - total)

        loop(BX, 2, body)

    def keep_wide(i, plane):
        wide[i] = plane

    for load in loads:
        load.wait()
    pack(0)
    pack(1)
    pl.semaphore_wait(barrier, count)

    start(fine_copies(0, 2))
    finish(fine_copies(0, 2))
    widen(1)
    coefficients()
    widen(0)
    put_coarse(0, down())
    start(deep_copies(0))
    finish(deep_copies(0))
    shape = (CX * nx, 16, BZ)
    row = iota(shape, 1)
    y = CY * gy + jnp.where(row < 10, row - 2, row - 18)
    z = CZ * gz + wrapped(iota(shape, 2), 128)
    inv2[...] = masked_inverse(coarse_field(1), None, y, z, 1)
    edge = jnp.zeros((16, BZ), F32)
    coarse[0] = edge
    coarse[CX * nx + 1] = edge
    solve_coarsest(coarse_field(0))
    up(keep_wide)

    sums[...] = jnp.zeros_like(sums)

    def first_image(x, value, image):
        p_out[x] = value
        image_out[x] = image
        own[2, x] = image
        sums[0] += own[0, x] * value
        sums[1] += image * value

    operate(first_image)
    pack(2)
    start(fine_copies(2, 1))
    gamma = jnp.sum(sums[0], axis=0, keepdims=True)
    delta = jnp.sum(sums[1], axis=0, keepdims=True)
    low = iota((1, BZ), 1) < 64
    gamma, delta = gamma + pltpu.roll(gamma, 64, 1), delta + pltpu.roll(delta, 64, 1)
    line_start(2, jnp.where(low, gamma, delta))
    finish(fine_copies(2, 1))
    widen(2)
    put_coarse(2, down())
    start(deep_copies(1))
    line_start(1, line_finish(2))
    finish(deep_copies(1))
    solve_coarsest(coarse_field(2))
    up(keep_wide)
    line_start(0, line_finish(1))

    def second_image(x, value, image):
        mw_out[x] = value
        nw_out[x] = image

    operate(second_image)
    total = line_finish(0)
    gamma = jnp.sum(jnp.where(low, total, 0.0), axis=1, keepdims=True)
    delta = jnp.sum(jnp.where(low, 0.0, total), axis=1, keepdims=True)
    alpha_out[...] = jnp.broadcast_to(gamma / delta, alpha_out.shape)


def call(sizes, right_side, coefficient):
    nx = sizes[0]
    block = jax.ShapeDtypeStruct((BX, BY, BZ), F32)
    any_spec = pl.BlockSpec(memory_space=pl.ANY)
    vmem_spec = pl.BlockSpec(memory_space=pltpu.VMEM)
    vmem = pltpu.VMEM
    return pl.pallas_call(
        functools.partial(kernel, sizes),
        out_shape=[block] * 4 + [jax.ShapeDtypeStruct((1, BZ), F32)],
        in_specs=[any_spec] * 2,
        out_specs=[vmem_spec] * 5,
        scratch_shapes=[
            vmem((3, BX, BY, BZ), F32),
            vmem((3, LX, LY, BZ), F32),
            vmem((2, 3, BX, 1, BZ), F32),
            vmem((2, 3, 3, LX, 1, BZ), F32),
            vmem((3, CX, 1, BZ), F32),
            vmem((3, 3, 3, CX * nx, 1, BZ), F32),
            vmem((LX, LY, 2 * BZ), F32),
            vmem((LX, LY, 2 * BZ), F32),
            vmem((LX, LY, 2 * BZ), F32),
            vmem((10, LY, 2 * BZ), F32),
            vmem((10, 16, BZ), F32),
            vmem((10, 16, BZ), F32),
            vmem((10, 16, BZ), F32),
            vmem((CX * nx, 16, BZ), F32),
            vmem((CX * nx + 2, 16, BZ), F32),
            vmem((10, LY, BZ), F32),
            vmem((CX, 16, BZ), F32),
            vmem((5, 16, BZ), F32),
            vmem((8, LY, BZ), F32),
            vmem((BZ, 2 * BZ), BF16),
            vmem((2 * BZ, BZ), BF16),
            vmem((2 * BZ, BZ), BF16),
            vmem((BZ, BZ), BF16),
            vmem((BZ, BZ), BF16),
            vmem((BZ, 2 * BZ), BF16),
            vmem((2, BY, BZ), F32),
            vmem((3, 1, BZ), F32),
            vmem((sizes[0], 1, BZ), F32),
            vmem((sizes[1], 1, BZ), F32),
            vmem((sizes[2], 1, BZ), F32),
            pltpu.SemaphoreType.DMA((2,)),
            pltpu.SemaphoreType.DMA((len(FINE),)),
            pltpu.SemaphoreType.DMA((len(FINE),)),
            pltpu.SemaphoreType.DMA((2, len(DEEP))),
            pltpu.SemaphoreType.DMA((2, len(DEEP))),
            pltpu.SemaphoreType.DMA((3, max(sizes))),
            pltpu.SemaphoreType.DMA((3, max(sizes))),
        ],
        compiler_params=pltpu.CompilerParams(collective_id=0, has_side_effects=True),
    )(right_side, coefficient)


def solution(mesh):
    sizes = tuple(mesh.shape[axis] for axis in ("gx", "gy", "gz"))

    def shards(right_side, coefficient):
        precond, image, mw, nw, alpha = call(sizes, right_side, coefficient)
        alpha = alpha[None]
        return (
            alpha * precond,
            right_side - alpha * image,
            precond - alpha * mw,
            image - alpha * nw,
        )

    spec = P("gx", "gy", "gz")
    return jax.shard_map(
        shards, mesh=mesh, in_specs=(spec, spec), out_specs=(spec,) * 4, check_vma=False
    )
```

```python
import functools

import jax
import jax.numpy as jnp
from jax import lax
from jax.experimental import pallas as pl
from jax.experimental.pallas import tpu as pltpu
from jax.sharding import PartitionSpec as P

MESH = pl.DeviceIdType.MESH
F32 = jnp.float32
BF16 = jnp.bfloat16

BX, BY, BZ = 12, 16, 128
CX, CY, CZ = 3, 4, 32
HX = 5
LX = BX + 2 * HX
LY = 32
FINE = [
    (dx, dy, dz)
    for dx in (-1, 0, 1)
    for dy in (-1, 0, 1)
    for dz in (-1, 0, 1)
    if (dx, dy, dz) != (0, 0, 0)
]
DEEP = [
    (dx, dy, dz)
    for dx in (-2, -1, 0, 1, 2)
    for dy in (-1, 0, 1)
    for dz in (-1, 0, 1)
    if (dx, dy, dz) != (0, 0, 0)
]
FINE.sort(key=lambda d: -sum(abs(s) for s in d))
DEEP.sort(key=lambda d: -sum(abs(s) for s in d))


def iota(shape, axis):
    return lax.broadcasted_iota(jnp.int32, shape, axis)


def split(values):
    high = values.astype(BF16)
    rest = values - high.astype(F32)
    middle = rest.astype(BF16)
    low = (rest - middle.astype(F32)).astype(BF16)
    return high, middle, low


def select_dot(values, table):
    high, middle, low = split(values)
    dot = functools.partial(jnp.dot, preferred_element_type=F32)
    return dot(low, table) + dot(middle, table) + dot(high, table)


def ones_where(condition):
    return jnp.where(condition, 1.0, 0.0).astype(BF16)


def wrapped(lane, size):
    return jnp.where(lane < size * 3 // 4, lane, lane - size)


def around(plane):
    rows, lanes = plane.shape[-2:]
    axis = plane.ndim - 2
    plane = plane + pltpu.roll(plane, 1, axis) + pltpu.roll(plane, rows - 1, axis)
    return plane + pltpu.roll(plane, 1, axis + 1) + pltpu.roll(plane, lanes - 1, axis + 1)


def loop(count, unroll, body):
    def step(i, carry):
        body(i)
        return carry

    lax.fori_loop(0, count, step, 0, unroll=unroll)


def kernel(
    sizes,
    g_in, c_in,
    p_out, image_out, mw_out, nw_out, alpha_out,
    own, ext, packed, halo, coarse_own, coarse_ext,
    wide, inv0, e0, rest0, inv1, g1, e1, inv2, coarse,
    t_fine, t_mid, p_mid, p_fine,
    m_pack, m_unpack, m_r0, m_r1, m_p1, m_p0,
    sums, line_own, line_0, line_1, line_2,
    fine_send, fine_recv, deep_send, deep_recv, line_send, line_recv, hello,
):
    nx, ny, nz = sizes
    gx, gy, gz = lax.axis_index("gx"), lax.axis_index("gy"), lax.axis_index("gz")

    def exists(d):
        checks = []
        for delta, at, count in zip(d, (gx, gy, gz), sizes):
            if delta < 0:
                checks.append(at >= -delta)
            if delta > 0:
                checks.append(at < count - delta)
        return functools.reduce(jnp.logical_and, checks)

    def device(d):
        return (gx + d[0], gy + d[1], gz + d[2])

    def along(axis, k):
        at = [gx, gy, gz]
        at[axis] = lax.rem(at[axis] + k, sizes[axis])
        return tuple(at)

    ext[...] = jnp.zeros_like(ext)
    halo[...] = jnp.zeros_like(halo)
    coarse_ext[...] = jnp.zeros_like(coarse_ext)

    barrier = pltpu.get_barrier_semaphore()
    greeted = [(axis, k) for axis in range(2) for k in range(1, sizes[axis])]
    greeted += [(2, k) for k in range(1, nz) if min(k, nz - k) <= 4]
    count = jnp.int32(len(greeted))
    for d in FINE:
        if sum(s != 0 for s in d) == 1:
            continue
        count = count + exists(d).astype(jnp.int32)

        @pl.when(exists(d))
        def _(d=d):
            pl.semaphore_signal(barrier, inc=1, device_id=device(d), device_id_type=MESH)

    for axis, k in greeted:
        pl.semaphore_signal(barrier, inc=1, device_id=along(axis, k), device_id_type=MESH)

    row, col = iota((BZ, 2 * BZ), 0), iota((BZ, 2 * BZ), 1)
    m_pack[...] = ones_where(row == jnp.where(col < BZ, col % 8, 120 + col % 8))
    row, col = iota((2 * BZ, BZ), 0), iota((2 * BZ, BZ), 1)
    m_unpack[...] = ones_where(col == jnp.where(row < BZ, 120 + row % 8, row % 8))
    m_r0[...] = ones_where(col == (jnp.where(row < 192, row, row - 256) >> 1) % 128)
    row, col = iota((BZ, BZ), 0), iota((BZ, BZ), 1)
    m_r1[...] = ones_where(jnp.logical_and(row < 64, (row >> 1) == col % 32))
    m_p1[...] = ones_where(row == (wrapped(col, 128) >> 1) % 128)
    row, col = iota((BZ, 2 * BZ), 0), iota((BZ, 2 * BZ), 1)
    m_p0[...] = ones_where(row == (wrapped(col, 256) >> 1) % 128)

    def pack(field):
        values = own[field].reshape(BX * BY, BZ)
        spread = select_dot(values, m_pack[...]).reshape(BX, BY, 2 * BZ)
        lane, row = iota((BX, BY, 2 * BZ), 2), iota((BX, BY, 2 * BZ), 1)
        spread = jnp.where((lane % 128) // 8 == row, spread, 0.0)
        flat = jnp.sum(spread, axis=1, keepdims=True)
        packed[0, field] = flat[:, :, :BZ]
        packed[1, field] = flat[:, :, BZ:]

    def fine_copies(first, count):
        fields = pl.ds(first, count)
        for n, (dx, dy, dz) in enumerate(FINE):
            source = {-1: pl.ds(0, HX), 0: pl.ds(0, BX), 1: pl.ds(BX - HX, HX)}[dx]
            target = {-1: pl.ds(HX + BX, HX), 0: pl.ds(HX, BX), 1: pl.ds(0, HX)}[dx]
            if dz == 0:
                rows = {-1: pl.ds(0, 8), 0: pl.ds(0, 16), 1: pl.ds(8, 8)}[dy]
                to = {-1: pl.ds(24, 8), 0: pl.ds(8, 16), 1: pl.ds(0, 8)}[dy]
                src, dst = own.at[fields, source, rows], ext.at[fields, target, to]
            else:
                src = packed.at[(dz + 1) // 2, fields, source]
                dst = halo.at[(1 - dz) // 2, fields, 1 - dy, target]
            yield n, (dx, dy, dz), pltpu.make_async_remote_copy(
                src_ref=src, dst_ref=dst, send_sem=fine_send.at[n], recv_sem=fine_recv.at[n],
                device_id=device((dx, dy, dz)), device_id_type=MESH,
            )

    def deep_copies(part):
        fields = pl.ds(0, 2) if part == 0 else pl.ds(2, 1)
        for n, (dx, dy, dz) in enumerate(DEEP):
            yield n, (dx, dy, dz), pltpu.make_async_remote_copy(
                src_ref=coarse_own.at[fields],
                dst_ref=coarse_ext.at[fields, 1 - dy, 1 - dz, pl.ds(CX * gx, CX)],
                send_sem=deep_send.at[part, n], recv_sem=deep_recv.at[part, n],
                device_id=device((dx, dy, dz)), device_id_type=MESH,
            )

    def start(copies):
        for n, d, copy in copies:
            @pl.when(exists(d))
            def _(copy=copy):
                copy.start()

    def finish(copies):
        copies = list(copies)
        for n, d, copy in copies:
            @pl.when(exists(tuple(-s for s in d)))
            def _(copy=copy):
                copy.wait_recv()
        for n, d, copy in copies:
            @pl.when(exists(d))
            def _(copy=copy):
                copy.wait_send()

    lines = (line_0, line_1, line_2)

    def line_copies(axis):
        me = (gx, gy, gz)[axis]
        for k in range(1, sizes[axis]):
            yield pltpu.make_async_remote_copy(
                src_ref=line_own.at[axis], dst_ref=lines[axis].at[me],
                send_sem=line_send.at[axis], recv_sem=line_recv.at[axis],
                device_id=along(axis, k), device_id_type=MESH,
            )

    def line_start(axis, row):
        line_own[axis] = row
        lines[axis][(gx, gy, gz)[axis]] = row
        for copy in line_copies(axis):
            copy.start()

    def line_finish(axis):
        rest = lines[axis].at[pl.ds(0, sizes[axis] - 1)]
        whole = pltpu.make_async_remote_copy(
            src_ref=rest, dst_ref=rest, send_sem=line_send.at[axis], recv_sem=line_recv.at[axis],
            device_id=along(axis, 1), device_id_type=MESH,
        )
        whole.wait_recv()
        whole.wait_send()
        return jnp.sum(lines[axis][...], axis=0)

    def widen(field):
        ext[field, HX : HX + BX, 8:24] = own[field]
        lane, row = iota((LY, BZ), 1), iota((LY, BZ), 0)
        fits = (lane // 8) == (row + 8) % 16
        sides = []
        for side in (0, 1):
            rows = jnp.concatenate(
                [
                    jnp.broadcast_to(halo[side, field, 0], (LX, 8, BZ)),
                    jnp.broadcast_to(halo[side, field, 1], (LX, 16, BZ)),
                    jnp.broadcast_to(halo[side, field, 2], (LX, 8, BZ)),
                ],
                axis=1,
            )
            sides.append(jnp.where(fits[None], rows, 0.0).reshape(LX * LY, BZ))
        outer = select_dot(sides[0], m_unpack[:BZ]) + select_dot(sides[1], m_unpack[BZ:])
        wide[:, :, :BZ] = ext[field]
        wide[:, :, BZ:] = outer.reshape(LX, LY, BZ)

    def restrict_fine():
        t_fine[...] = select_dot(rest0[...].reshape(10 * LY, 2 * BZ), m_r0[...]).reshape(10, LY, BZ)
        return 0.5 * (t_fine[:, pl.ds(0, 16, stride=2)] + t_fine[:, pl.ds(1, 16, stride=2)])

    def restrict_mid(values):
        pairs = values.reshape(CX, 2, 16, BZ)
        pairs = pairs[:, 0] + pairs[:, 1]
        t_mid[...] = select_dot(pairs.reshape(CX * 16, BZ), m_r1[...]).reshape(CX, 16, BZ)
        cells = 0.5 * (t_mid[:, pl.ds(0, 8, stride=2)] + t_mid[:, pl.ds(1, 8, stride=2)])
        lane, row = iota((8, BZ), 1), iota((8, BZ), 0)
        return jnp.sum(jnp.where((lane // 32 == row - 2)[None], cells, 0.0), axis=1, keepdims=True)

    def put_coarse(field, cells):
        coarse_own[field] = cells
        coarse_ext[field, 1, 1, pl.ds(CX * gx, CX)] = cells

    def coarse_field(field):
        shape = (CX * nx, 16, BZ)
        lane, row = iota((16, BZ), 1), iota((16, BZ), 0)
        y = jnp.where(row < 10, row - 2, row - 18)
        slot, group = (y + 4) // 4, (row + 2) % 4
        total = None
        for dz in (-1, 0, 1):
            rows = jnp.zeros(shape, F32)
            for dy in (-1, 0, 1):
                fits = jnp.logical_and(slot == dy + 1, lane // 32 == group)
                taken = jnp.broadcast_to(coarse_ext[field, dy + 1, dz + 1], shape)
                rows = jnp.where(fits[None], taken, rows)
            rows = rows + pltpu.roll(rows, 32, 2)
            rows = rows + pltpu.roll(rows, 64, 2)
            rows = jnp.where((lane // 32 == dz % 4)[None], rows, 0.0)
            total = rows if total is None else total + rows
        return total

    def masked_inverse(values, x, y, z, scale):
        ok = jnp.logical_and(y >= 0, y < scale * CY * ny)
        ok = jnp.logical_and(ok, jnp.logical_and(z >= 0, z < scale * CZ * nz))
        if x is not None:
            ok = jnp.logical_and(ok, jnp.logical_and(x >= 0, x < scale * CX * nx))
        return jnp.where(ok, 0.6 / (26.0 + values), 0.0)

    def coefficients():
        lane, row = iota((LY, 2 * BZ), 1), iota((LY, 2 * BZ), 0)
        y, z = BY * gy + row - 8, BZ * gz + wrapped(lane, 256)

        def body(i):
            inv0[i] = masked_inverse(wide[i], BX * gx + i - HX, y, z, 4)

        loop(LX, 2, body)

        def pairs(j):
            rest0[j] = wide[2 * j + 1] + wide[2 * j + 2]

        loop(10, 2, pairs)
        c1 = restrict_fine()
        put_coarse(1, restrict_mid(c1[2:8]))
        shape = (10, 16, BZ)
        x = 2 * CX * gx + iota(shape, 0) - 2
        y = 2 * CY * gy + iota(shape, 1) - 4
        z = 2 * CZ * gz + wrapped(iota(shape, 2), 128)
        inv1[...] = masked_inverse(c1, x, y, z, 2)

    def down():
        def guess(i):
            e0[i] = inv0[i] * wide[i]

        loop(LX, 2, guess)

        def rest(j):
            i = 2 * j
            e_0, e_1, e_2, e_3 = e0[i], e0[i + 1], e0[i + 2], e0[i + 3]
            middle = e_1 + e_2
            total = around(e_0 + middle + (middle + e_3)) - middle
            rest0[j] = 0.4 * (wide[i + 1] + wide[i + 2]) + total

        loop(10, 2, rest)
        right = restrict_fine()
        g1[...] = right
        first = inv1[...] * right
        e1[...] = first
        total = first[1:7] + first[2:8] + first[3:9]
        remainder = 0.4 * right[2:8] + around(total) - first[2:8]
        return restrict_mid(remainder)

    def solve_coarsest(right):
        inverse = inv2[...]
        edge = jnp.zeros((1, 16, BZ), F32)
        e = inverse * right
        for _ in range(3):
            padded = jnp.concatenate([edge, e, edge], axis=0)
            total = around(padded[:-2] + padded[1:-1] + padded[2:])
            e = 0.4 * e + inverse * (right + total - e)
        coarse[pl.ds(1, CX * nx)] = e

    def up(keep):
        near = coarse[pl.ds(CX * gx, CX + 2)][:, :8]
        p_mid[:, pl.ds(0, 8, stride=2)] = near
        p_mid[:, pl.ds(1, 8, stride=2)] = near
        rise = select_dot(p_mid[...].reshape(5 * 16, BZ), m_p1[...]).reshape(5, 1, 16, BZ)
        rise = jnp.broadcast_to(rise, (5, 2, 16, BZ)).reshape(10, 16, BZ)
        e = e1[...] + rise
        total = around(e[0:8] + e[1:9] + e[2:10])
        e = 0.4 * e[1:9] + inv1[1:9] * (g1[1:9] + total - e[1:9])
        p_fine[:, pl.ds(0, 16, stride=2)] = e
        p_fine[:, pl.ds(1, 16, stride=2)] = e
        rest0[pl.ds(0, 8)] = select_dot(p_fine[...].reshape(8 * LY, BZ), m_p0[...]).reshape(8, LY, 2 * BZ)

        def add(j):
            i = 2 * j + 3
            e0[i] = e0[i] + rest0[j]
            e0[i + 1] = e0[i + 1] + rest0[j]

        loop(8, 2, add)

        def smooth(k):
            i = k + 4
            e = e0[i]
            total = around(e0[i - 1] + e + e0[i + 1])
            keep(i, 0.4 * e + inv0[i] * (wide[i] + total - e))

        loop(14, 2, smooth)

    def operate(keep):
        def body(x):
            i = x + HX
            value = wide[i]
            total = around(wide[i - 1] + value + wide[i + 1])
            value, total = value[8:24, :BZ], total[8:24, :BZ]
            keep(x, value, (27.0 + own[1, x]) * value - total)

        loop(BX, 2, body)

    def keep_wide(i, plane):
        wide[i] = plane

    own[0] = g_in[...]
    own[1] = c_in[...]
    pack(0)
    pack(1)
    pl.semaphore_wait(barrier, count)

    start(fine_copies(0, 2))
    far = [k for k in (4, nz - 4) if nz > 8]
    for k in far:
        pl.semaphore_signal(hello, inc=1, device_id=along(2, k), device_id_type=MESH)
    finish(fine_copies(0, 2))
    widen(1)
    coefficients()
    widen(0)
    put_coarse(0, down())
    start(deep_copies(0))
    finish(deep_copies(0))
    if far:
        pl.semaphore_wait(hello, len(far))
    shape = (CX * nx, 16, BZ)
    row = iota(shape, 1)
    y = CY * gy + jnp.where(row < 10, row - 2, row - 18)
    z = CZ * gz + wrapped(iota(shape, 2), 128)
    inv2[...] = masked_inverse(coarse_field(1), None, y, z, 1)
    edge = jnp.zeros((16, BZ), F32)
    coarse[0] = edge
    coarse[CX * nx + 1] = edge
    solve_coarsest(coarse_field(0))
    up(keep_wide)

    sums[...] = jnp.zeros_like(sums)

    def first_image(x, value, image):
        p_out[x] = value
        image_out[x] = image
        own[2, x] = image
        sums[0] += own[0, x] * value
        sums[1] += image * value

    operate(first_image)
    pack(2)
    start(fine_copies(2, 1))
    gamma = jnp.sum(sums[0], axis=0, keepdims=True)
    delta = jnp.sum(sums[1], axis=0, keepdims=True)
    low = iota((1, BZ), 1) < 64
    gamma, delta = gamma + pltpu.roll(gamma, 64, 1), delta + pltpu.roll(delta, 64, 1)
    line_start(0, jnp.where(low, gamma, delta))
    finish(fine_copies(2, 1))
    line_start(1, line_finish(0))
    widen(2)
    put_coarse(2, down())
    start(deep_copies(1))
    line_start(2, line_finish(1))
    finish(deep_copies(1))
    solve_coarsest(coarse_field(2))
    up(keep_wide)

    def second_image(x, value, image):
        mw_out[x] = value
        nw_out[x] = image

    operate(second_image)
    total = line_finish(2)
    gamma = jnp.sum(jnp.where(low, total, 0.0), axis=1, keepdims=True)
    delta = jnp.sum(jnp.where(low, 0.0, total), axis=1, keepdims=True)
    alpha_out[...] = jnp.broadcast_to(gamma / delta, alpha_out.shape)


def call(sizes, right_side, coefficient):
    nx = sizes[0]
    block = jax.ShapeDtypeStruct((BX, BY, BZ), F32)
    vmem_spec = pl.BlockSpec(memory_space=pltpu.VMEM)
    vmem = pltpu.VMEM
    return pl.pallas_call(
        functools.partial(kernel, sizes),
        out_shape=[block] * 4 + [jax.ShapeDtypeStruct((1, BZ), F32)],
        in_specs=[vmem_spec] * 2,
        out_specs=[vmem_spec] * 5,
        scratch_shapes=[
            vmem((3, BX, BY, BZ), F32),
            vmem((3, LX, LY, BZ), F32),
            vmem((2, 3, BX, 1, BZ), F32),
            vmem((2, 3, 3, LX, 1, BZ), F32),
            vmem((3, CX, 1, BZ), F32),
            vmem((3, 3, 3, CX * nx, 1, BZ), F32),
            vmem((LX, LY, 2 * BZ), F32),
            vmem((LX, LY, 2 * BZ), F32),
            vmem((LX, LY, 2 * BZ), F32),
            vmem((10, LY, 2 * BZ), F32),
            vmem((10, 16, BZ), F32),
            vmem((10, 16, BZ), F32),
            vmem((10, 16, BZ), F32),
            vmem((CX * nx, 16, BZ), F32),
            vmem((CX * nx + 2, 16, BZ), F32),
            vmem((10, LY, BZ), F32),
            vmem((CX, 16, BZ), F32),
            vmem((5, 16, BZ), F32),
            vmem((8, LY, BZ), F32),
            vmem((BZ, 2 * BZ), BF16),
            vmem((2 * BZ, BZ), BF16),
            vmem((2 * BZ, BZ), BF16),
            vmem((BZ, BZ), BF16),
            vmem((BZ, BZ), BF16),
            vmem((BZ, 2 * BZ), BF16),
            vmem((2, BY, BZ), F32),
            vmem((3, 1, BZ), F32),
            vmem((sizes[0], 1, BZ), F32),
            vmem((sizes[1], 1, BZ), F32),
            vmem((sizes[2], 1, BZ), F32),
            pltpu.SemaphoreType.DMA((len(FINE),)),
            pltpu.SemaphoreType.DMA((len(FINE),)),
            pltpu.SemaphoreType.DMA((2, len(DEEP))),
            pltpu.SemaphoreType.DMA((2, len(DEEP))),
            pltpu.SemaphoreType.DMA((3,)),
            pltpu.SemaphoreType.DMA((3,)),
            pltpu.SemaphoreType.REGULAR,
        ],
        compiler_params=pltpu.CompilerParams(
            collective_id=0, has_side_effects=True, vmem_limit_bytes=16 * 1024 * 1024
        ),
    )(right_side, coefficient)


def solution(mesh):
    sizes = tuple(mesh.shape[axis] for axis in ("gx", "gy", "gz"))

    def shards(right_side, coefficient):
        precond, image, mw, nw, alpha = call(sizes, right_side, coefficient)
        alpha = alpha[None]
        return (
            alpha * precond,
            right_side - alpha * image,
            precond - alpha * mw,
            image - alpha * nw,
        )

    spec = P("gx", "gy", "gz")
    return jax.shard_map(
        shards, mesh=mesh, in_specs=(spec, spec), out_specs=(spec,) * 4, check_vma=False
    )
```

```python
import functools

import jax
import jax.numpy as jnp
from jax import lax
from jax.experimental import pallas as pl
from jax.experimental.pallas import tpu as pltpu
from jax.sharding import PartitionSpec as P

MESH = pl.DeviceIdType.MESH
F32 = jnp.float32
BF16 = jnp.bfloat16

BX, BY, BZ = 12, 16, 128
CX, CY, CZ = 3, 4, 32
HX = 5
LX = BX + 2 * HX
LY = 32
FINE = [
    (dx, dy, dz)
    for dx in (-1, 0, 1)
    for dy in (-1, 0, 1)
    for dz in (-1, 0, 1)
    if (dx, dy, dz) != (0, 0, 0)
]
DEEP = [
    (dx, dy, dz)
    for dx in (-2, -1, 0, 1, 2)
    for dy in (-1, 0, 1)
    for dz in (-1, 0, 1)
    if (dx, dy, dz) != (0, 0, 0)
]
FINE.sort(key=lambda d: -sum(abs(s) for s in d))
DEEP.sort(key=lambda d: -sum(abs(s) for s in d))


def iota(shape, axis):
    return lax.broadcasted_iota(jnp.int32, shape, axis)


def split(values):
    high = values.astype(BF16)
    rest = values - high.astype(F32)
    middle = rest.astype(BF16)
    low = (rest - middle.astype(F32)).astype(BF16)
    return high, middle, low


def select_dot(values, table):
    high, middle, low = split(values)
    dot = functools.partial(jnp.dot, preferred_element_type=F32)
    return dot(low, table) + dot(middle, table) + dot(high, table)


def ones_where(condition):
    return jnp.where(condition, 1.0, 0.0).astype(BF16)


def wrapped(lane, size):
    return jnp.where(lane < size * 3 // 4, lane, lane - size)


def around(plane):
    rows, lanes = plane.shape[-2:]
    axis = plane.ndim - 2
    plane = plane + pltpu.roll(plane, 1, axis) + pltpu.roll(plane, rows - 1, axis)
    return plane + pltpu.roll(plane, 1, axis + 1) + pltpu.roll(plane, lanes - 1, axis + 1)


def loop(count, unroll, body):
    def step(i, carry):
        body(i)
        return carry

    lax.fori_loop(0, count, step, 0, unroll=unroll)


def kernel(
    sizes,
    g_in, c_in,
    p_out, image_out, mw_out, nw_out, alpha_out,
    own, ext, packed, halo, coarse_own, coarse_ext, again_own, again_ext,
    wide, inv0, e0, rest0, inv1, g1, e1, inv2, coarse,
    t_fine, t_mid, p_mid, p_fine,
    m_pack, m_unpack, m_r0, m_r1, m_p1, m_p0,
    sums, line_own, line_0, line_1, line_2,
    load_sem, fine_send, fine_recv, deep_send, deep_recv, line_send, line_recv, hello,
):
    nx, ny, nz = sizes
    gx, gy, gz = lax.axis_index("gx"), lax.axis_index("gy"), lax.axis_index("gz")

    def exists(d):
        checks = []
        for delta, at, count in zip(d, (gx, gy, gz), sizes):
            if delta < 0:
                checks.append(at >= -delta)
            if delta > 0:
                checks.append(at < count - delta)
        return functools.reduce(jnp.logical_and, checks)

    def device(d):
        return (gx + d[0], gy + d[1], gz + d[2])

    def along(axis, k):
        at = [gx, gy, gz]
        at[axis] = lax.rem(at[axis] + k, sizes[axis])
        return tuple(at)

    loads = [pltpu.make_async_copy(r, own.at[n], load_sem.at[n]) for n, r in enumerate((g_in, c_in))]
    for load in loads:
        load.start()

    ext[...] = jnp.zeros_like(ext)
    halo[...] = jnp.zeros_like(halo)
    coarse_ext[...] = jnp.zeros_like(coarse_ext)
    again_ext[...] = jnp.zeros_like(again_ext)

    barrier = pltpu.get_barrier_semaphore()
    greeted = [(axis, k) for axis in range(2) for k in range(1, sizes[axis])]
    greeted += [(2, k) for k in range(1, nz) if min(k, nz - k) <= 4]
    count = jnp.int32(len(greeted))
    for d in FINE:
        if sum(s != 0 for s in d) == 1:
            continue
        count = count + exists(d).astype(jnp.int32)

        @pl.when(exists(d))
        def _(d=d):
            pl.semaphore_signal(barrier, inc=1, device_id=device(d), device_id_type=MESH)

    for axis, k in greeted:
        pl.semaphore_signal(barrier, inc=1, device_id=along(axis, k), device_id_type=MESH)

    row, col = iota((BZ, 2 * BZ), 0), iota((BZ, 2 * BZ), 1)
    m_pack[...] = ones_where(row == jnp.where(col < BZ, col % 8, 120 + col % 8))
    row, col = iota((2 * BZ, BZ), 0), iota((2 * BZ, BZ), 1)
    m_unpack[...] = ones_where(col == jnp.where(row < BZ, 120 + row % 8, row % 8))
    m_r0[...] = ones_where(col == (jnp.where(row < 192, row, row - 256) >> 1) % 128)
    row, col = iota((BZ, BZ), 0), iota((BZ, BZ), 1)
    m_r1[...] = ones_where(jnp.logical_and(row < 64, (row >> 1) == col % 32))
    m_p1[...] = ones_where(row == (wrapped(col, 128) >> 1) % 128)
    row, col = iota((BZ, 2 * BZ), 0), iota((BZ, 2 * BZ), 1)
    m_p0[...] = ones_where(row == (wrapped(col, 256) >> 1) % 128)

    def pack(field):
        values = own[field].reshape(BX * BY, BZ)
        spread = select_dot(values, m_pack[...]).reshape(BX, BY, 2 * BZ)
        lane, row = iota((BX, BY, 2 * BZ), 2), iota((BX, BY, 2 * BZ), 1)
        spread = jnp.where((lane % 128) // 8 == row, spread, 0.0)
        flat = jnp.sum(spread, axis=1, keepdims=True)
        packed[0, field] = flat[:, :, :BZ]
        packed[1, field] = flat[:, :, BZ:]

    def fine_copies(part):
        first, count = ((0, 2), (2, 1))[part]
        fields = pl.ds(first, count)
        for n, (dx, dy, dz) in enumerate(FINE):
            source = {-1: pl.ds(0, HX), 0: pl.ds(0, BX), 1: pl.ds(BX - HX, HX)}[dx]
            target = {-1: pl.ds(HX + BX, HX), 0: pl.ds(HX, BX), 1: pl.ds(0, HX)}[dx]
            if dz == 0:
                rows = {-1: pl.ds(0, 8), 0: pl.ds(0, 16), 1: pl.ds(8, 8)}[dy]
                to = {-1: pl.ds(24, 8), 0: pl.ds(8, 16), 1: pl.ds(0, 8)}[dy]
                src, dst = own.at[fields, source, rows], ext.at[fields, target, to]
            else:
                src = packed.at[(dz + 1) // 2, fields, source]
                dst = halo.at[(1 - dz) // 2, fields, 1 - dy, target]
            yield n, (dx, dy, dz), pltpu.make_async_remote_copy(
                src_ref=src, dst_ref=dst, send_sem=fine_send.at[part, n], recv_sem=fine_recv.at[part, n],
                device_id=device((dx, dy, dz)), device_id_type=MESH,
            )

    def deep_copies(part):
        source, target = ((coarse_own, coarse_ext), (again_own, again_ext))[part]
        for n, (dx, dy, dz) in enumerate(DEEP):
            yield n, (dx, dy, dz), pltpu.make_async_remote_copy(
                src_ref=source,
                dst_ref=target.at[1 - dy, 1 - dz, pl.ds(CX * gx, CX)],
                send_sem=deep_send.at[part, n], recv_sem=deep_recv.at[part, n],
                device_id=device((dx, dy, dz)), device_id_type=MESH,
            )

    def start(copies):
        for n, d, copy in copies:
            @pl.when(exists(d))
            def _(copy=copy):
                copy.start()

    def finish(copies):
        for n, d, copy in copies:
            @pl.when(exists(tuple(-s for s in d)))
            def _(copy=copy):
                copy.wait_recv()

    def sent(copies):
        for n, d, copy in copies:
            @pl.when(exists(d))
            def _(copy=copy):
                copy.wait_send()

    lines = (line_0, line_1, line_2)

    def line_copies(axis):
        me = (gx, gy, gz)[axis]
        for k in range(1, sizes[axis]):
            yield pltpu.make_async_remote_copy(
                src_ref=line_own.at[axis], dst_ref=lines[axis].at[me],
                send_sem=line_send.at[axis], recv_sem=line_recv.at[axis],
                device_id=along(axis, k), device_id_type=MESH,
            )

    def line_start(axis, row):
        line_own[axis] = row
        lines[axis][(gx, gy, gz)[axis]] = row
        for copy in line_copies(axis):
            copy.start()

    def line_whole(axis):
        rest = lines[axis].at[pl.ds(0, sizes[axis] - 1)]
        return pltpu.make_async_remote_copy(
            src_ref=rest, dst_ref=rest, send_sem=line_send.at[axis], recv_sem=line_recv.at[axis],
            device_id=along(axis, 1), device_id_type=MESH,
        )

    def line_finish(axis):
        line_whole(axis).wait_recv()
        return jnp.sum(lines[axis][...], axis=0)

    def widen(field):
        ext[field, HX : HX + BX, 8:24] = own[field]
        lane, row = iota((LY, BZ), 1), iota((LY, BZ), 0)
        fits = (lane // 8) == (row + 8) % 16
        sides = []
        for side in (0, 1):
            rows = jnp.concatenate(
                [
                    jnp.broadcast_to(halo[side, field, 0], (LX, 8, BZ)),
                    jnp.broadcast_to(halo[side, field, 1], (LX, 16, BZ)),
                    jnp.broadcast_to(halo[side, field, 2], (LX, 8, BZ)),
                ],
                axis=1,
            )
            sides.append(jnp.where(fits[None], rows, 0.0).reshape(LX * LY, BZ))
        outer = select_dot(sides[0], m_unpack[:BZ]) + select_dot(sides[1], m_unpack[BZ:])
        wide[:, :, :BZ] = ext[field]
        wide[:, :, BZ:] = outer.reshape(LX, LY, BZ)

    def restrict_fine():
        t_fine[...] = select_dot(rest0[...].reshape(10 * LY, 2 * BZ), m_r0[...]).reshape(10, LY, BZ)
        return 0.5 * (t_fine[:, pl.ds(0, 16, stride=2)] + t_fine[:, pl.ds(1, 16, stride=2)])

    def restrict_mid(values):
        pairs = values.reshape(CX, 2, 16, BZ)
        pairs = pairs[:, 0] + pairs[:, 1]
        t_mid[...] = select_dot(pairs.reshape(CX * 16, BZ), m_r1[...]).reshape(CX, 16, BZ)
        cells = 0.5 * (t_mid[:, pl.ds(0, 8, stride=2)] + t_mid[:, pl.ds(1, 8, stride=2)])
        lane, row = iota((8, BZ), 1), iota((8, BZ), 0)
        return jnp.sum(jnp.where((lane // 32 == row - 2)[None], cells, 0.0), axis=1, keepdims=True)

    def put_coarse(field, cells):
        if field == 2:
            again_own[...] = cells
            again_ext[1, 1, pl.ds(CX * gx, CX)] = cells
        else:
            coarse_own[:, field] = cells
            coarse_ext[1, 1, pl.ds(CX * gx, CX), field] = cells

    def coarse_field(field):
        shape = (CX * nx, 16, BZ)
        lane, row = iota((16, BZ), 1), iota((16, BZ), 0)
        y = jnp.where(row < 10, row - 2, row - 18)
        slot, group = (y + 4) // 4, (row + 2) % 4
        total = None
        for dz in (-1, 0, 1):
            rows = jnp.zeros(shape, F32)
            for dy in (-1, 0, 1):
                fits = jnp.logical_and(slot == dy + 1, lane // 32 == group)
                if field == 2:
                    taken = again_ext[dy + 1, dz + 1]
                else:
                    taken = coarse_ext[dy + 1, dz + 1, :, field]
                taken = jnp.broadcast_to(taken, shape)
                rows = jnp.where(fits[None], taken, rows)
            rows = rows + pltpu.roll(rows, 32, 2)
            rows = rows + pltpu.roll(rows, 64, 2)
            rows = jnp.where((lane // 32 == dz % 4)[None], rows, 0.0)
            total = rows if total is None else total + rows
        return total

    def masked_inverse(values, x, y, z, scale):
        ok = jnp.logical_and(y >= 0, y < scale * CY * ny)
        ok = jnp.logical_and(ok, jnp.logical_and(z >= 0, z < scale * CZ * nz))
        if x is not None:
            ok = jnp.logical_and(ok, jnp.logical_and(x >= 0, x < scale * CX * nx))
        return jnp.where(ok, 0.6 / (26.0 + values), 0.0)

    def coefficients():
        lane, row = iota((LY, 2 * BZ), 1), iota((LY, 2 * BZ), 0)
        y, z = BY * gy + row - 8, BZ * gz + wrapped(lane, 256)

        def body(i):
            inv0[i] = masked_inverse(wide[i], BX * gx + i - HX, y, z, 4)

        loop(LX, 22, body)

        def pairs(j):
            rest0[j] = wide[2 * j + 1] + wide[2 * j + 2]

        loop(10, 10, pairs)
        c1 = restrict_fine()
        put_coarse(1, restrict_mid(c1[2:8]))
        shape = (10, 16, BZ)
        x = 2 * CX * gx + iota(shape, 0) - 2
        y = 2 * CY * gy + iota(shape, 1) - 4
        z = 2 * CZ * gz + wrapped(iota(shape, 2), 128)
        inv1[...] = masked_inverse(c1, x, y, z, 2)

    def down():
        def guess(i):
            e0[i] = inv0[i] * wide[i]

        loop(LX, 22, guess)

        def rest(j):
            i = 2 * j
            e_0, e_1, e_2, e_3 = e0[i], e0[i + 1], e0[i + 2], e0[i + 3]
            middle = e_1 + e_2
            total = around(e_0 + middle + (middle + e_3)) - middle
            rest0[j] = 0.4 * (wide[i + 1] + wide[i + 2]) + total

        loop(10, 10, rest)
        right = restrict_fine()
        g1[...] = right
        first = inv1[...] * right
        e1[...] = first
        total = first[1:7] + first[2:8] + first[3:9]
        remainder = 0.4 * right[2:8] + around(total) - first[2:8]
        return restrict_mid(remainder)

    def solve_coarsest(right):
        inverse = inv2[...]
        edge = jnp.zeros((1, 16, BZ), F32)
        e = inverse * right
        for _ in range(3):
            padded = jnp.concatenate([edge, e, edge], axis=0)
            total = around(padded[:-2] + padded[1:-1] + padded[2:])
            e = 0.4 * e + inverse * (right + total - e)
        coarse[pl.ds(1, CX * nx)] = e

    def up(keep):
        near = coarse[pl.ds(CX * gx, CX + 2)][:, :8]
        p_mid[:, pl.ds(0, 8, stride=2)] = near
        p_mid[:, pl.ds(1, 8, stride=2)] = near
        rise = select_dot(p_mid[...].reshape(5 * 16, BZ), m_p1[...]).reshape(5, 1, 16, BZ)
        rise = jnp.broadcast_to(rise, (5, 2, 16, BZ)).reshape(10, 16, BZ)
        e = e1[...] + rise
        total = around(e[0:8] + e[1:9] + e[2:10])
        e = 0.4 * e[1:9] + inv1[1:9] * (g1[1:9] + total - e[1:9])
        p_fine[:, pl.ds(0, 16, stride=2)] = e
        p_fine[:, pl.ds(1, 16, stride=2)] = e
        rest0[pl.ds(0, 8)] = select_dot(p_fine[...].reshape(8 * LY, BZ), m_p0[...]).reshape(8, LY, 2 * BZ)

        def add(j):
            i = 2 * j + 3
            e0[i] = e0[i] + rest0[j]
            e0[i + 1] = e0[i + 1] + rest0[j]

        loop(8, 8, add)

        def smooth(k):
            i = k + 4
            e = e0[i]
            total = around(e0[i - 1] + e + e0[i + 1])
            keep(i, 0.4 * e + inv0[i] * (wide[i] + total - e))

        loop(14, 14, smooth)

    def operate(keep):
        def body(x):
            i = x + HX
            value = wide[i]
            total = around(wide[i - 1] + value + wide[i + 1])
            value, total = value[8:24, :BZ], total[8:24, :BZ]
            keep(x, value, (27.0 + own[1, x]) * value - total)

        loop(BX, 12, body)

    def keep_wide(i, plane):
        wide[i] = plane

    for load in loads:
        load.wait()
    pack(0)
    pack(1)
    pl.semaphore_wait(barrier, count)

    start(fine_copies(0))
    far = [k for k in (4, nz - 4) if nz > 8]
    for k in far:
        pl.semaphore_signal(hello, inc=1, device_id=along(2, k), device_id_type=MESH)
    finish(fine_copies(0))
    widen(1)
    coefficients()
    widen(0)
    put_coarse(0, down())
    start(deep_copies(0))
    finish(deep_copies(0))
    if far:
        pl.semaphore_wait(hello, len(far))
    shape = (CX * nx, 16, BZ)
    row = iota(shape, 1)
    y = CY * gy + jnp.where(row < 10, row - 2, row - 18)
    z = CZ * gz + wrapped(iota(shape, 2), 128)
    inv2[...] = masked_inverse(coarse_field(1), None, y, z, 1)
    edge = jnp.zeros((16, BZ), F32)
    coarse[0] = edge
    coarse[CX * nx + 1] = edge
    solve_coarsest(coarse_field(0))
    up(keep_wide)

    sums[...] = jnp.zeros_like(sums)

    def first_image(x, value, image):
        p_out[x] = value
        image_out[x] = image
        own[2, x] = image
        sums[0] += own[0, x] * value
        sums[1] += image * value

    operate(first_image)
    pack(2)
    start(fine_copies(1))
    gamma = jnp.sum(sums[0], axis=0, keepdims=True)
    delta = jnp.sum(sums[1], axis=0, keepdims=True)
    low = iota((1, BZ), 1) < 64
    gamma, delta = gamma + pltpu.roll(gamma, 64, 1), delta + pltpu.roll(delta, 64, 1)
    line_start(0, jnp.where(low, gamma, delta))
    finish(fine_copies(1))
    line_start(1, line_finish(0))
    widen(2)
    put_coarse(2, down())
    start(deep_copies(1))
    line_start(2, line_finish(1))
    finish(deep_copies(1))
    solve_coarsest(coarse_field(2))
    up(keep_wide)

    def second_image(x, value, image):
        mw_out[x] = value
        nw_out[x] = image

    operate(second_image)
    for part in range(2):
        sent(fine_copies(part))
        sent(deep_copies(part))
    for axis in range(3):
        line_whole(axis).wait_send()
    total = line_finish(2)
    gamma = jnp.sum(jnp.where(low, total, 0.0), axis=1, keepdims=True)
    delta = jnp.sum(jnp.where(low, 0.0, total), axis=1, keepdims=True)
    alpha_out[...] = jnp.broadcast_to(gamma / delta, alpha_out.shape)


def call(sizes, right_side, coefficient):
    nx = sizes[0]
    block = jax.ShapeDtypeStruct((BX, BY, BZ), F32)
    vmem_spec = pl.BlockSpec(memory_space=pltpu.VMEM)
    vmem = pltpu.VMEM
    return pl.pallas_call(
        functools.partial(kernel, sizes),
        out_shape=[block] * 4 + [jax.ShapeDtypeStruct((1, BZ), F32)],
        in_specs=[pl.BlockSpec(memory_space=pltpu.HBM)] * 2,
        out_specs=[vmem_spec] * 5,
        scratch_shapes=[
            vmem((3, BX, BY, BZ), F32),
            vmem((3, LX, LY, BZ), F32),
            vmem((2, 3, BX, 1, BZ), F32),
            vmem((2, 3, 3, LX, 1, BZ), F32),
            vmem((CX, 2, 1, BZ), F32),
            vmem((3, 3, CX * nx, 2, 1, BZ), F32),
            vmem((CX, 1, BZ), F32),
            vmem((3, 3, CX * nx, 1, BZ), F32),
            vmem((LX, LY, 2 * BZ), F32),
            vmem((LX, LY, 2 * BZ), F32),
            vmem((LX, LY, 2 * BZ), F32),
            vmem((10, LY, 2 * BZ), F32),
            vmem((10, 16, BZ), F32),
            vmem((10, 16, BZ), F32),
            vmem((10, 16, BZ), F32),
            vmem((CX * nx, 16, BZ), F32),
            vmem((CX * nx + 2, 16, BZ), F32),
            vmem((10, LY, BZ), F32),
            vmem((CX, 16, BZ), F32),
            vmem((5, 16, BZ), F32),
            vmem((8, LY, BZ), F32),
            vmem((BZ, 2 * BZ), BF16),
            vmem((2 * BZ, BZ), BF16),
            vmem((2 * BZ, BZ), BF16),
            vmem((BZ, BZ), BF16),
            vmem((BZ, BZ), BF16),
            vmem((BZ, 2 * BZ), BF16),
            vmem((2, BY, BZ), F32),
            vmem((3, 1, BZ), F32),
            vmem((sizes[0], 1, BZ), F32),
            vmem((sizes[1], 1, BZ), F32),
            vmem((sizes[2], 1, BZ), F32),
            pltpu.SemaphoreType.DMA((2,)),
            pltpu.SemaphoreType.DMA((2, len(FINE))),
            pltpu.SemaphoreType.DMA((2, len(FINE))),
            pltpu.SemaphoreType.DMA((2, len(DEEP))),
            pltpu.SemaphoreType.DMA((2, len(DEEP))),
            pltpu.SemaphoreType.DMA((3,)),
            pltpu.SemaphoreType.DMA((3,)),
            pltpu.SemaphoreType.REGULAR,
        ],
        compiler_params=pltpu.CompilerParams(
            collective_id=0, has_side_effects=True, vmem_limit_bytes=16 * 1024 * 1024
        ),
    )(right_side, coefficient)


def solution(mesh):
    sizes = tuple(mesh.shape[axis] for axis in ("gx", "gy", "gz"))

    def shards(right_side, coefficient):
        held = [pltpu.with_memory_space_constraint(a, pltpu.HBM) for a in (right_side, coefficient)]
        precond, image, mw, nw, alpha = call(sizes, *held)
        alpha = alpha[None]
        return (
            alpha * precond,
            right_side - alpha * image,
            precond - alpha * mw,
            image - alpha * nw,
        )

    spec = P("gx", "gy", "gz")
    return jax.shard_map(
        shards, mesh=mesh, in_specs=(spec, spec), out_specs=(spec,) * 4, check_vma=False
    )
```

```python
import functools

import jax
import jax.numpy as jnp
from jax import lax
from jax.experimental import pallas as pl
from jax.experimental.pallas import tpu as pltpu
from jax.sharding import PartitionSpec as P

MESH = pl.DeviceIdType.MESH
F32 = jnp.float32
BF16 = jnp.bfloat16

BX, BY, BZ = 12, 16, 128
CX, CY, CZ = 3, 4, 32
HX = 5
LX = BX + 2 * HX
LY = 32
FINE = [
    (dx, dy, dz)
    for dx in (-1, 0, 1)
    for dy in (-1, 0, 1)
    for dz in (-1, 0, 1)
    if (dx, dy, dz) != (0, 0, 0)
]
DEEP = [
    (dx, dy, dz)
    for dx in (-2, -1, 0, 1, 2)
    for dy in (-1, 0, 1)
    for dz in (-1, 0, 1)
    if (dx, dy, dz) != (0, 0, 0)
]
FINE.sort(key=lambda d: -sum(abs(s) for s in d))
DEEP.sort(key=lambda d: -sum(abs(s) for s in d))


def iota(shape, axis):
    return lax.broadcasted_iota(jnp.int32, shape, axis)


def split(values):
    high = values.astype(BF16)
    rest = values - high.astype(F32)
    middle = rest.astype(BF16)
    low = (rest - middle.astype(F32)).astype(BF16)
    return high, middle, low


def select_dot(values, table):
    high, middle, low = split(values)
    dot = functools.partial(jnp.dot, preferred_element_type=F32)
    return dot(low, table) + dot(middle, table) + dot(high, table)


def ones_where(condition):
    return jnp.where(condition, 1.0, 0.0).astype(BF16)


def wrapped(lane, size):
    return jnp.where(lane < size * 3 // 4, lane, lane - size)


def around(plane):
    rows, lanes = plane.shape[-2:]
    axis = plane.ndim - 2
    plane = plane + pltpu.roll(plane, 1, axis) + pltpu.roll(plane, rows - 1, axis)
    return plane + pltpu.roll(plane, 1, axis + 1) + pltpu.roll(plane, lanes - 1, axis + 1)


def loop(count, unroll, body):
    def step(i, carry):
        body(i)
        return carry

    lax.fori_loop(0, count, step, 0, unroll=unroll)


def kernel(
    sizes,
    g_in, c_in,
    p_out, image_out, mw_out, nw_out, alpha_out,
    own, ext, packed, halo, coarse_own, coarse_ext, again_own, again_ext,
    wide, inv0, e0, rest0, inv1, g1, e1, inv2, coarse,
    t_fine, t_mid, p_mid, p_fine,
    m_pack, m_unpack, m_r0, m_r1, m_p1, m_p0,
    sums, line_own, line_0, line_1,
    load_sem, fine_send, fine_recv, deep_send, deep_recv, line_send, line_recv, hello,
):
    nx, ny, nz = sizes
    gx, gy, gz = lax.axis_index("gx"), lax.axis_index("gy"), lax.axis_index("gz")

    def exists(d):
        checks = []
        for delta, at, count in zip(d, (gx, gy, gz), sizes):
            if delta < 0:
                checks.append(at >= -delta)
            if delta > 0:
                checks.append(at < count - delta)
        return functools.reduce(jnp.logical_and, checks)

    def device(d):
        return (gx + d[0], gy + d[1], gz + d[2])

    def across(i, j):
        return (lax.rem(gx + i, nx), lax.rem(gy + j, ny), gz)

    def along(axis, k):
        at = [gx, gy, gz]
        at[axis] = lax.rem(at[axis] + k, sizes[axis])
        return tuple(at)

    loads = [pltpu.make_async_copy(r, own.at[n], load_sem.at[n]) for n, r in enumerate((g_in, c_in))]
    for load in loads:
        load.start()

    ext[...] = jnp.zeros_like(ext)
    halo[...] = jnp.zeros_like(halo)
    coarse_ext[...] = jnp.zeros_like(coarse_ext)
    again_ext[...] = jnp.zeros_like(again_ext)

    barrier = pltpu.get_barrier_semaphore()
    greeted = [(axis, k) for axis in range(2) for k in range(1, sizes[axis])]
    greeted += [(2, k) for k in range(1, nz) if min(k, nz - k) <= 4]
    count = jnp.int32(len(greeted))
    for d in FINE:
        if sum(s != 0 for s in d) == 1:
            continue
        count = count + exists(d).astype(jnp.int32)

        @pl.when(exists(d))
        def _(d=d):
            pl.semaphore_signal(barrier, inc=1, device_id=device(d), device_id_type=MESH)

    for axis, k in greeted:
        pl.semaphore_signal(barrier, inc=1, device_id=along(axis, k), device_id_type=MESH)

    row, col = iota((BZ, 2 * BZ), 0), iota((BZ, 2 * BZ), 1)
    m_pack[...] = ones_where(row == jnp.where(col < BZ, col % 8, 120 + col % 8))
    row, col = iota((2 * BZ, BZ), 0), iota((2 * BZ, BZ), 1)
    m_unpack[...] = ones_where(col == jnp.where(row < BZ, 120 + row % 8, row % 8))
    m_r0[...] = ones_where(col == (jnp.where(row < 192, row, row - 256) >> 1) % 128)
    row, col = iota((BZ, BZ), 0), iota((BZ, BZ), 1)
    m_r1[...] = ones_where(jnp.logical_and(row < 64, (row >> 1) == col % 32))
    m_p1[...] = ones_where(row == (wrapped(col, 128) >> 1) % 128)
    row, col = iota((BZ, 2 * BZ), 0), iota((BZ, 2 * BZ), 1)
    m_p0[...] = ones_where(row == (wrapped(col, 256) >> 1) % 128)

    def pack(field):
        values = own[field].reshape(BX * BY, BZ)
        spread = select_dot(values, m_pack[...]).reshape(BX, BY, 2 * BZ)
        lane, row = iota((BX, BY, 2 * BZ), 2), iota((BX, BY, 2 * BZ), 1)
        spread = jnp.where((lane % 128) // 8 == row, spread, 0.0)
        flat = jnp.sum(spread, axis=1, keepdims=True)
        packed[0, field] = flat[:, :, :BZ]
        packed[1, field] = flat[:, :, BZ:]

    def fine_copies(part):
        first, count = ((0, 2), (2, 1))[part]
        fields = pl.ds(first, count)
        for n, (dx, dy, dz) in enumerate(FINE):
            source = {-1: pl.ds(0, HX), 0: pl.ds(0, BX), 1: pl.ds(BX - HX, HX)}[dx]
            target = {-1: pl.ds(HX + BX, HX), 0: pl.ds(HX, BX), 1: pl.ds(0, HX)}[dx]
            if dz == 0:
                rows = {-1: pl.ds(0, 8), 0: pl.ds(0, 16), 1: pl.ds(8, 8)}[dy]
                to = {-1: pl.ds(24, 8), 0: pl.ds(8, 16), 1: pl.ds(0, 8)}[dy]
                src, dst = own.at[fields, source, rows], ext.at[fields, target, to]
            else:
                src = packed.at[(dz + 1) // 2, fields, source]
                dst = halo.at[(1 - dz) // 2, fields, 1 - dy, target]
            yield n, (dx, dy, dz), pltpu.make_async_remote_copy(
                src_ref=src, dst_ref=dst, send_sem=fine_send.at[part, n], recv_sem=fine_recv.at[part, n],
                device_id=device((dx, dy, dz)), device_id_type=MESH,
            )

    def deep_copies(part):
        source, target = ((coarse_own, coarse_ext), (again_own, again_ext))[part]
        for n, (dx, dy, dz) in enumerate(DEEP):
            yield n, (dx, dy, dz), pltpu.make_async_remote_copy(
                src_ref=source,
                dst_ref=target.at[1 - dy, 1 - dz, pl.ds(CX * gx, CX)],
                send_sem=deep_send.at[part, n], recv_sem=deep_recv.at[part, n],
                device_id=device((dx, dy, dz)), device_id_type=MESH,
            )

    def start(copies):
        for n, d, copy in copies:
            @pl.when(exists(d))
            def _(copy=copy):
                copy.start()

    def finish(copies):
        for n, d, copy in copies:
            @pl.when(exists(tuple(-s for s in d)))
            def _(copy=copy):
                copy.wait_recv()

    def sent(copies):
        for n, d, copy in copies:
            @pl.when(exists(d))
            def _(copy=copy):
                copy.wait_send()

    planes = [(i, j) for i in range(nx) for j in range(ny) if (i, j) != (0, 0)]
    phases = (line_0, line_1)
    places = (gx * ny + gy, gz)
    targets = ([across(i, j) for i, j in planes], [along(2, k) for k in range(1, nz)])

    def line_copy(phase, source, target, device_id):
        return pltpu.make_async_remote_copy(
            src_ref=source, dst_ref=target,
            send_sem=line_send.at[phase], recv_sem=line_recv.at[phase],
            device_id=device_id, device_id_type=MESH,
        )

    def line_start(phase, row):
        line_own[phase] = row
        target = phases[phase].at[places[phase]]
        phases[phase][places[phase]] = row
        for device_id in targets[phase]:
            line_copy(phase, line_own.at[phase], target, device_id).start()

    def line_whole(phase):
        rest = phases[phase].at[pl.ds(0, len(targets[phase]))]
        return line_copy(phase, rest, rest, targets[phase][0])

    def line_finish(phase):
        line_whole(phase).wait_recv()
        return jnp.sum(phases[phase][...], axis=0)

    def widen(field):
        ext[field, HX : HX + BX, 8:24] = own[field]
        lane, row = iota((LY, BZ), 1), iota((LY, BZ), 0)
        fits = (lane // 8) == (row + 8) % 16
        sides = []
        for side in (0, 1):
            rows = jnp.concatenate(
                [
                    jnp.broadcast_to(halo[side, field, 0], (LX, 8, BZ)),
                    jnp.broadcast_to(halo[side, field, 1], (LX, 16, BZ)),
                    jnp.broadcast_to(halo[side, field, 2], (LX, 8, BZ)),
                ],
                axis=1,
            )
            sides.append(jnp.where(fits[None], rows, 0.0).reshape(LX * LY, BZ))
        outer = select_dot(sides[0], m_unpack[:BZ]) + select_dot(sides[1], m_unpack[BZ:])
        wide[:, :, :BZ] = ext[field]
        wide[:, :, BZ:] = outer.reshape(LX, LY, BZ)

    def restrict_fine():
        t_fine[...] = select_dot(rest0[...].reshape(10 * LY, 2 * BZ), m_r0[...]).reshape(10, LY, BZ)
        return 0.5 * (t_fine[:, pl.ds(0, 16, stride=2)] + t_fine[:, pl.ds(1, 16, stride=2)])

    def restrict_mid(values):
        pairs = values.reshape(CX, 2, 16, BZ)
        pairs = pairs[:, 0] + pairs[:, 1]
        t_mid[...] = select_dot(pairs.reshape(CX * 16, BZ), m_r1[...]).reshape(CX, 16, BZ)
        cells = 0.5 * (t_mid[:, pl.ds(0, 8, stride=2)] + t_mid[:, pl.ds(1, 8, stride=2)])
        lane, row = iota((8, BZ), 1), iota((8, BZ), 0)
        return jnp.sum(jnp.where((lane // 32 == row - 2)[None], cells, 0.0), axis=1, keepdims=True)

    def put_coarse(field, cells):
        if field == 2:
            again_own[...] = cells
            again_ext[1, 1, pl.ds(CX * gx, CX)] = cells
        else:
            coarse_own[:, field] = cells
            coarse_ext[1, 1, pl.ds(CX * gx, CX), field] = cells

    def coarse_field(field):
        shape = (CX * nx, 16, BZ)
        lane, row = iota((16, BZ), 1), iota((16, BZ), 0)
        y = jnp.where(row < 10, row - 2, row - 18)
        slot, group = (y + 4) // 4, (row + 2) % 4
        total = None
        for dz in (-1, 0, 1):
            rows = jnp.zeros(shape, F32)
            for dy in (-1, 0, 1):
                fits = jnp.logical_and(slot == dy + 1, lane // 32 == group)
                if field == 2:
                    taken = again_ext[dy + 1, dz + 1]
                else:
                    taken = coarse_ext[dy + 1, dz + 1, :, field]
                taken = jnp.broadcast_to(taken, shape)
                rows = jnp.where(fits[None], taken, rows)
            rows = rows + pltpu.roll(rows, 32, 2)
            rows = rows + pltpu.roll(rows, 64, 2)
            rows = jnp.where((lane // 32 == dz % 4)[None], rows, 0.0)
            total = rows if total is None else total + rows
        return total

    def masked_inverse(values, x, y, z, scale):
        ok = jnp.logical_and(y >= 0, y < scale * CY * ny)
        ok = jnp.logical_and(ok, jnp.logical_and(z >= 0, z < scale * CZ * nz))
        if x is not None:
            ok = jnp.logical_and(ok, jnp.logical_and(x >= 0, x < scale * CX * nx))
        return jnp.where(ok, 0.6 / (26.0 + values), 0.0)

    def coefficients():
        lane, row = iota((LY, 2 * BZ), 1), iota((LY, 2 * BZ), 0)
        y, z = BY * gy + row - 8, BZ * gz + wrapped(lane, 256)

        def body(i):
            inv0[i] = masked_inverse(wide[i], BX * gx + i - HX, y, z, 4)

        loop(LX, 22, body)

        def pairs(j):
            rest0[j] = wide[2 * j + 1] + wide[2 * j + 2]

        loop(10, 10, pairs)
        c1 = restrict_fine()
        put_coarse(1, restrict_mid(c1[2:8]))
        shape = (10, 16, BZ)
        x = 2 * CX * gx + iota(shape, 0) - 2
        y = 2 * CY * gy + iota(shape, 1) - 4
        z = 2 * CZ * gz + wrapped(iota(shape, 2), 128)
        inv1[...] = masked_inverse(c1, x, y, z, 2)

    def down():
        def guess(i):
            e0[i] = inv0[i] * wide[i]

        loop(LX, 22, guess)

        def rest(j):
            i = 2 * j
            e_0, e_1, e_2, e_3 = e0[i], e0[i + 1], e0[i + 2], e0[i + 3]
            middle = e_1 + e_2
            total = around(e_0 + middle + (middle + e_3)) - middle
            rest0[j] = 0.4 * (wide[i + 1] + wide[i + 2]) + total

        loop(10, 10, rest)
        right = restrict_fine()
        g1[...] = right
        first = inv1[...] * right
        e1[...] = first
        total = first[1:7] + first[2:8] + first[3:9]
        remainder = 0.4 * right[2:8] + around(total) - first[2:8]
        return restrict_mid(remainder)

    def solve_coarsest(right):
        inverse = inv2[...]
        edge = jnp.zeros((1, 16, BZ), F32)
        e = inverse * right
        for _ in range(3):
            padded = jnp.concatenate([edge, e, edge], axis=0)
            total = around(padded[:-2] + padded[1:-1] + padded[2:])
            e = 0.4 * e + inverse * (right + total - e)
        coarse[pl.ds(1, CX * nx)] = e

    def up(keep):
        near = coarse[pl.ds(CX * gx, CX + 2)][:, :8]
        p_mid[:, pl.ds(0, 8, stride=2)] = near
        p_mid[:, pl.ds(1, 8, stride=2)] = near
        rise = select_dot(p_mid[...].reshape(5 * 16, BZ), m_p1[...]).reshape(5, 1, 16, BZ)
        rise = jnp.broadcast_to(rise, (5, 2, 16, BZ)).reshape(10, 16, BZ)
        e = e1[...] + rise
        total = around(e[0:8] + e[1:9] + e[2:10])
        e = 0.4 * e[1:9] + inv1[1:9] * (g1[1:9] + total - e[1:9])
        p_fine[:, pl.ds(0, 16, stride=2)] = e
        p_fine[:, pl.ds(1, 16, stride=2)] = e
        rest0[pl.ds(0, 8)] = select_dot(p_fine[...].reshape(8 * LY, BZ), m_p0[...]).reshape(8, LY, 2 * BZ)

        def add(j):
            i = 2 * j + 3
            e0[i] = e0[i] + rest0[j]
            e0[i + 1] = e0[i + 1] + rest0[j]

        loop(8, 8, add)

        def smooth(k):
            i = k + 4
            e = e0[i]
            total = around(e0[i - 1] + e + e0[i + 1])
            keep(i, 0.4 * e + inv0[i] * (wide[i] + total - e))

        loop(14, 14, smooth)

    def operate(keep):
        def body(x):
            i = x + HX
            value = wide[i]
            total = around(wide[i - 1] + value + wide[i + 1])
            value, total = value[8:24, :BZ], total[8:24, :BZ]
            keep(x, value, (27.0 + own[1, x]) * value - total)

        loop(BX, 12, body)

    def keep_wide(i, plane):
        wide[i] = plane

    for load in loads:
        load.wait()
    pack(0)
    pack(1)
    pl.semaphore_wait(barrier, count)

    start(fine_copies(0))
    far = [(2, k) for k in (4, nz - 4) if nz > 8] + [(0, k) for k in range(1, nx)]
    for axis, k in far:
        pl.semaphore_signal(hello, inc=1, device_id=along(axis, k), device_id_type=MESH)
    finish(fine_copies(0))
    widen(1)
    coefficients()
    widen(0)
    put_coarse(0, down())
    start(deep_copies(0))
    finish(deep_copies(0))
    if far:
        pl.semaphore_wait(hello, len(far))
    shape = (CX * nx, 16, BZ)
    row = iota(shape, 1)
    y = CY * gy + jnp.where(row < 10, row - 2, row - 18)
    z = CZ * gz + wrapped(iota(shape, 2), 128)
    inv2[...] = masked_inverse(coarse_field(1), None, y, z, 1)
    edge = jnp.zeros((16, BZ), F32)
    coarse[0] = edge
    coarse[CX * nx + 1] = edge
    solve_coarsest(coarse_field(0))
    up(keep_wide)

    sums[...] = jnp.zeros_like(sums)

    def first_image(x, value, image):
        p_out[x] = value
        image_out[x] = image
        own[2, x] = image
        sums[0] += own[0, x] * value
        sums[1] += image * value

    operate(first_image)
    gamma = jnp.sum(sums[0], axis=0, keepdims=True)
    delta = jnp.sum(sums[1], axis=0, keepdims=True)
    low = iota((1, BZ), 1) < 64
    gamma, delta = gamma + pltpu.roll(gamma, 64, 1), delta + pltpu.roll(delta, 64, 1)
    line_start(0, jnp.where(low, gamma, delta))
    start(copy for copy in fine_copies(1) if copy[1][2] == 0)
    pack(2)
    start(copy for copy in fine_copies(1) if copy[1][2] != 0)
    finish(fine_copies(1))
    widen(2)
    put_coarse(2, down())
    start(deep_copies(1))
    line_start(1, line_finish(0))
    finish(deep_copies(1))
    solve_coarsest(coarse_field(2))
    up(keep_wide)

    def second_image(x, value, image):
        mw_out[x] = value
        nw_out[x] = image

    operate(second_image)
    for part in range(2):
        sent(fine_copies(part))
        sent(deep_copies(part))
    for phase in range(2):
        line_whole(phase).wait_send()
    total = line_finish(1)
    gamma = jnp.sum(jnp.where(low, total, 0.0), axis=1, keepdims=True)
    delta = jnp.sum(jnp.where(low, 0.0, total), axis=1, keepdims=True)
    alpha_out[...] = jnp.broadcast_to(gamma / delta, alpha_out.shape)


def call(sizes, right_side, coefficient):
    nx = sizes[0]
    block = jax.ShapeDtypeStruct((BX, BY, BZ), F32)
    vmem_spec = pl.BlockSpec(memory_space=pltpu.VMEM)
    vmem = pltpu.VMEM
    return pl.pallas_call(
        functools.partial(kernel, sizes),
        out_shape=[block] * 4 + [jax.ShapeDtypeStruct((1, BZ), F32)],
        in_specs=[pl.BlockSpec(memory_space=pltpu.HBM)] * 2,
        out_specs=[vmem_spec] * 5,
        scratch_shapes=[
            vmem((3, BX, BY, BZ), F32),
            vmem((3, LX, LY, BZ), F32),
            vmem((2, 3, BX, 1, BZ), F32),
            vmem((2, 3, 3, LX, 1, BZ), F32),
            vmem((CX, 2, 1, BZ), F32),
            vmem((3, 3, CX * nx, 2, 1, BZ), F32),
            vmem((CX, 1, BZ), F32),
            vmem((3, 3, CX * nx, 1, BZ), F32),
            vmem((LX, LY, 2 * BZ), F32),
            vmem((LX, LY, 2 * BZ), F32),
            vmem((LX, LY, 2 * BZ), F32),
            vmem((10, LY, 2 * BZ), F32),
            vmem((10, 16, BZ), F32),
            vmem((10, 16, BZ), F32),
            vmem((10, 16, BZ), F32),
            vmem((CX * nx, 16, BZ), F32),
            vmem((CX * nx + 2, 16, BZ), F32),
            vmem((10, LY, BZ), F32),
            vmem((CX, 16, BZ), F32),
            vmem((5, 16, BZ), F32),
            vmem((8, LY, BZ), F32),
            vmem((BZ, 2 * BZ), BF16),
            vmem((2 * BZ, BZ), BF16),
            vmem((2 * BZ, BZ), BF16),
            vmem((BZ, BZ), BF16),
            vmem((BZ, BZ), BF16),
            vmem((BZ, 2 * BZ), BF16),
            vmem((2, BY, BZ), F32),
            vmem((2, 1, BZ), F32),
            vmem((nx * sizes[1], 1, BZ), F32),
            vmem((sizes[2], 1, BZ), F32),
            pltpu.SemaphoreType.DMA((2,)),
            pltpu.SemaphoreType.DMA((2, len(FINE))),
            pltpu.SemaphoreType.DMA((2, len(FINE))),
            pltpu.SemaphoreType.DMA((2, len(DEEP))),
            pltpu.SemaphoreType.DMA((2, len(DEEP))),
            pltpu.SemaphoreType.DMA((2,)),
            pltpu.SemaphoreType.DMA((2,)),
            pltpu.SemaphoreType.REGULAR,
        ],
        compiler_params=pltpu.CompilerParams(
            collective_id=0, has_side_effects=True, vmem_limit_bytes=16 * 1024 * 1024
        ),
    )(right_side, coefficient)


def solution(mesh):
    sizes = tuple(mesh.shape[axis] for axis in ("gx", "gy", "gz"))

    def shards(right_side, coefficient):
        held = [pltpu.with_memory_space_constraint(a, pltpu.HBM) for a in (right_side, coefficient)]
        precond, image, mw, nw, alpha = call(sizes, *held)
        alpha = alpha[None]
        return (
            alpha * precond,
            right_side - alpha * image,
            precond - alpha * mw,
            image - alpha * nw,
        )

    spec = P("gx", "gy", "gz")
    return jax.shard_map(
        shards, mesh=mesh, in_specs=(spec, spec), out_specs=(spec,) * 4, check_vma=False
    )
```

```python
import functools

import jax
import jax.numpy as jnp
from jax import lax
from jax.experimental import pallas as pl
from jax.experimental.pallas import tpu as pltpu
from jax.sharding import PartitionSpec as P

MESH = pl.DeviceIdType.MESH
F32 = jnp.float32
BF16 = jnp.bfloat16

BX, BY, BZ = 12, 16, 128
CX, CY, CZ = 3, 4, 32
HX = 5
LX = BX + 2 * HX
LY = 32
FINE = [
    (dx, dy, dz)
    for dx in (-1, 0, 1)
    for dy in (-1, 0, 1)
    for dz in (-1, 0, 1)
    if (dx, dy, dz) != (0, 0, 0)
]
DEEP = [
    (dx, dy, dz)
    for dx in (-2, -1, 0, 1, 2)
    for dy in (-1, 0, 1)
    for dz in (-1, 0, 1)
    if (dx, dy, dz) != (0, 0, 0)
]
FINE.sort(key=lambda d: -sum(abs(s) for s in d))
DEEP.sort(key=lambda d: -sum(abs(s) for s in d))


def iota(shape, axis):
    return lax.broadcasted_iota(jnp.int32, shape, axis)


def split(values):
    high = values.astype(BF16)
    rest = values - high.astype(F32)
    middle = rest.astype(BF16)
    low = (rest - middle.astype(F32)).astype(BF16)
    return high, middle, low


def select_dot(values, table):
    high, middle, low = split(values)
    dot = functools.partial(jnp.dot, preferred_element_type=F32)
    return dot(low, table) + dot(middle, table) + dot(high, table)


def ones_where(condition):
    return jnp.where(condition, 1.0, 0.0).astype(BF16)


def wrapped(lane, size):
    return jnp.where(lane < size * 3 // 4, lane, lane - size)


def around(plane):
    rows, lanes = plane.shape[-2:]
    axis = plane.ndim - 2
    plane = plane + pltpu.roll(plane, 1, axis) + pltpu.roll(plane, rows - 1, axis)
    return plane + pltpu.roll(plane, 1, axis + 1) + pltpu.roll(plane, lanes - 1, axis + 1)


def loop(count, unroll, body):
    def step(i, carry):
        body(i)
        return carry

    lax.fori_loop(0, count, step, 0, unroll=unroll)


def kernel(
    sizes,
    g_in, c_in,
    p_out, image_out, mw_out, nw_out, alpha_out,
    own, ext, packed, halo, coarse_own, coarse_ext, again_own, again_ext,
    wide, inv0, e0, rest0, inv1, g1, e1, inv2, coarse,
    t_fine, t_mid, p_mid, p_fine,
    m_pack, m_unpack, m_r0, m_r1, m_p1, m_p0,
    sums, line_own, line_0, line_1,
    load_sem, fine_send, fine_recv, deep_send, deep_recv, line_send, line_recv, hello,
):
    nx, ny, nz = sizes
    gx, gy, gz = lax.axis_index("gx"), lax.axis_index("gy"), lax.axis_index("gz")

    def exists(d):
        checks = []
        for delta, at, count in zip(d, (gx, gy, gz), sizes):
            if delta < 0:
                checks.append(at >= -delta)
            if delta > 0:
                checks.append(at < count - delta)
        return functools.reduce(jnp.logical_and, checks)

    def device(d):
        return (gx + d[0], gy + d[1], gz + d[2])

    def across(i, j):
        return (lax.rem(gx + i, nx), lax.rem(gy + j, ny), gz)

    def along(axis, k):
        at = [gx, gy, gz]
        at[axis] = lax.rem(at[axis] + k, sizes[axis])
        return tuple(at)

    loads = [pltpu.make_async_copy(r, own.at[n], load_sem.at[n]) for n, r in enumerate((g_in, c_in))]
    for load in loads:
        load.start()

    ext[...] = jnp.zeros_like(ext)
    halo[...] = jnp.zeros_like(halo)
    coarse_ext[...] = jnp.zeros_like(coarse_ext)
    again_ext[...] = jnp.zeros_like(again_ext)

    barrier = pltpu.get_barrier_semaphore()
    greeted = [(axis, k) for axis in range(2) for k in range(1, sizes[axis])]
    greeted += [(2, k) for k in range(1, nz) if min(k, nz - k) <= 4]
    count = jnp.int32(len(greeted))
    for d in FINE:
        if sum(s != 0 for s in d) == 1:
            continue
        count = count + exists(d).astype(jnp.int32)

        @pl.when(exists(d))
        def _(d=d):
            pl.semaphore_signal(barrier, inc=1, device_id=device(d), device_id_type=MESH)

    for axis, k in greeted:
        pl.semaphore_signal(barrier, inc=1, device_id=along(axis, k), device_id_type=MESH)

    row, col = iota((BZ, 2 * BZ), 0), iota((BZ, 2 * BZ), 1)
    m_pack[...] = ones_where(row == jnp.where(col < BZ, col % 8, 120 + col % 8))
    row, col = iota((2 * BZ, BZ), 0), iota((2 * BZ, BZ), 1)
    m_unpack[...] = ones_where(col == jnp.where(row < BZ, 120 + row % 8, row % 8))
    m_r0[...] = ones_where(col == (jnp.where(row < 192, row, row - 256) >> 1) % 128)
    row, col = iota((BZ, BZ), 0), iota((BZ, BZ), 1)
    m_r1[...] = ones_where(jnp.logical_and(row < 64, (row >> 1) == col % 32))
    m_p1[...] = ones_where(row == (wrapped(col, 128) >> 1) % 128)
    row, col = iota((BZ, 2 * BZ), 0), iota((BZ, 2 * BZ), 1)
    m_p0[...] = ones_where(row == (wrapped(col, 256) >> 1) % 128)

    def pack(field):
        values = own[field].reshape(BX * BY, BZ)
        spread = select_dot(values, m_pack[...]).reshape(BX, BY, 2 * BZ)
        lane, row = iota((BX, BY, 2 * BZ), 2), iota((BX, BY, 2 * BZ), 1)
        spread = jnp.where((lane % 128) // 8 == row, spread, 0.0)
        flat = jnp.sum(spread, axis=1, keepdims=True)
        packed[0, field] = flat[:, :, :BZ]
        packed[1, field] = flat[:, :, BZ:]

    def fine_copies(field):
        for n, (dx, dy, dz) in enumerate(FINE):
            source = {-1: pl.ds(0, HX), 0: pl.ds(0, BX), 1: pl.ds(BX - HX, HX)}[dx]
            target = {-1: pl.ds(HX + BX, HX), 0: pl.ds(HX, BX), 1: pl.ds(0, HX)}[dx]
            if dz == 0:
                rows = {-1: pl.ds(0, 8), 0: pl.ds(0, 16), 1: pl.ds(8, 8)}[dy]
                to = {-1: pl.ds(24, 8), 0: pl.ds(8, 16), 1: pl.ds(0, 8)}[dy]
                src, dst = own.at[field, source, rows], ext.at[field, target, to]
            else:
                src = packed.at[(dz + 1) // 2, field, source]
                dst = halo.at[(1 - dz) // 2, field, 1 - dy, target]
            yield n, (dx, dy, dz), pltpu.make_async_remote_copy(
                src_ref=src, dst_ref=dst, send_sem=fine_send.at[field, n], recv_sem=fine_recv.at[field, n],
                device_id=device((dx, dy, dz)), device_id_type=MESH,
            )

    def deep_copies(part):
        source, target = ((coarse_own, coarse_ext), (again_own, again_ext))[part]
        for n, (dx, dy, dz) in enumerate(DEEP):
            yield n, (dx, dy, dz), pltpu.make_async_remote_copy(
                src_ref=source,
                dst_ref=target.at[1 - dy, 1 - dz, pl.ds(CX * gx, CX)],
                send_sem=deep_send.at[part, n], recv_sem=deep_recv.at[part, n],
                device_id=device((dx, dy, dz)), device_id_type=MESH,
            )

    def start(copies):
        for n, d, copy in copies:
            @pl.when(exists(d))
            def _(copy=copy):
                copy.start()

    def finish(copies):
        for n, d, copy in copies:
            @pl.when(exists(tuple(-s for s in d)))
            def _(copy=copy):
                copy.wait_recv()

    def sent(copies):
        for n, d, copy in copies:
            @pl.when(exists(d))
            def _(copy=copy):
                copy.wait_send()

    planes = [(i, j) for i in range(nx) for j in range(ny) if (i, j) != (0, 0)]
    phases = (line_0, line_1)
    places = (gx * ny + gy, gz)
    targets = ([across(i, j) for i, j in planes], [along(2, k) for k in range(1, nz)])

    def line_copy(phase, source, target, device_id):
        return pltpu.make_async_remote_copy(
            src_ref=source, dst_ref=target,
            send_sem=line_send.at[phase], recv_sem=line_recv.at[phase],
            device_id=device_id, device_id_type=MESH,
        )

    def line_start(phase, row):
        line_own[phase] = row
        target = phases[phase].at[places[phase]]
        phases[phase][places[phase]] = row
        for device_id in targets[phase]:
            line_copy(phase, line_own.at[phase], target, device_id).start()

    def line_whole(phase):
        rest = phases[phase].at[pl.ds(0, len(targets[phase]))]
        return line_copy(phase, rest, rest, targets[phase][0])

    def line_finish(phase):
        line_whole(phase).wait_recv()
        return jnp.sum(phases[phase][...], axis=0)

    def widen(field):
        ext[field, HX : HX + BX, 8:24] = own[field]
        lane, row = iota((LY, BZ), 1), iota((LY, BZ), 0)
        fits = (lane // 8) == (row + 8) % 16
        sides = []
        for side in (0, 1):
            rows = jnp.concatenate(
                [
                    jnp.broadcast_to(halo[side, field, 0], (LX, 8, BZ)),
                    jnp.broadcast_to(halo[side, field, 1], (LX, 16, BZ)),
                    jnp.broadcast_to(halo[side, field, 2], (LX, 8, BZ)),
                ],
                axis=1,
            )
            sides.append(jnp.where(fits[None], rows, 0.0).reshape(LX * LY, BZ))
        outer = select_dot(sides[0], m_unpack[:BZ]) + select_dot(sides[1], m_unpack[BZ:])
        wide[:, :, :BZ] = ext[field]
        wide[:, :, BZ:] = outer.reshape(LX, LY, BZ)

    def restrict_fine():
        t_fine[...] = select_dot(rest0[...].reshape(10 * LY, 2 * BZ), m_r0[...]).reshape(10, LY, BZ)
        return 0.5 * (t_fine[:, pl.ds(0, 16, stride=2)] + t_fine[:, pl.ds(1, 16, stride=2)])

    def restrict_mid(values):
        pairs = values.reshape(CX, 2, 16, BZ)
        pairs = pairs[:, 0] + pairs[:, 1]
        t_mid[...] = select_dot(pairs.reshape(CX * 16, BZ), m_r1[...]).reshape(CX, 16, BZ)
        cells = 0.5 * (t_mid[:, pl.ds(0, 8, stride=2)] + t_mid[:, pl.ds(1, 8, stride=2)])
        lane, row = iota((8, BZ), 1), iota((8, BZ), 0)
        return jnp.sum(jnp.where((lane // 32 == row - 2)[None], cells, 0.0), axis=1, keepdims=True)

    def put_coarse(field, cells):
        if field == 2:
            again_own[...] = cells
            again_ext[1, 1, pl.ds(CX * gx, CX)] = cells
        else:
            coarse_own[:, field] = cells
            coarse_ext[1, 1, pl.ds(CX * gx, CX), field] = cells

    def coarse_field(field):
        shape = (CX * nx, 16, BZ)
        lane, row = iota((16, BZ), 1), iota((16, BZ), 0)
        y = jnp.where(row < 10, row - 2, row - 18)
        slot, group = (y + 4) // 4, (row + 2) % 4
        total = None
        for dz in (-1, 0, 1):
            rows = jnp.zeros(shape, F32)
            for dy in (-1, 0, 1):
                fits = jnp.logical_and(slot == dy + 1, lane // 32 == group)
                if field == 2:
                    taken = again_ext[dy + 1, dz + 1]
                else:
                    taken = coarse_ext[dy + 1, dz + 1, :, field]
                taken = jnp.broadcast_to(taken, shape)
                rows = jnp.where(fits[None], taken, rows)
            rows = rows + pltpu.roll(rows, 32, 2)
            rows = rows + pltpu.roll(rows, 64, 2)
            rows = jnp.where((lane // 32 == dz % 4)[None], rows, 0.0)
            total = rows if total is None else total + rows
        return total

    def masked_inverse(values, x, y, z, scale):
        ok = jnp.logical_and(y >= 0, y < scale * CY * ny)
        ok = jnp.logical_and(ok, jnp.logical_and(z >= 0, z < scale * CZ * nz))
        if x is not None:
            ok = jnp.logical_and(ok, jnp.logical_and(x >= 0, x < scale * CX * nx))
        return jnp.where(ok, 0.6 / (26.0 + values), 0.0)

    def coefficients():
        lane, row = iota((LY, 2 * BZ), 1), iota((LY, 2 * BZ), 0)
        y, z = BY * gy + row - 8, BZ * gz + wrapped(lane, 256)

        def body(i):
            inv0[i] = masked_inverse(wide[i], BX * gx + i - HX, y, z, 4)

        loop(LX, 22, body)

        def pairs(j):
            rest0[j] = wide[2 * j + 1] + wide[2 * j + 2]

        loop(10, 10, pairs)
        c1 = restrict_fine()
        put_coarse(1, restrict_mid(c1[2:8]))
        shape = (10, 16, BZ)
        x = 2 * CX * gx + iota(shape, 0) - 2
        y = 2 * CY * gy + iota(shape, 1) - 4
        z = 2 * CZ * gz + wrapped(iota(shape, 2), 128)
        inv1[...] = masked_inverse(c1, x, y, z, 2)

    def down():
        def guess(i):
            e0[i] = inv0[i] * wide[i]

        loop(LX, 22, guess)

        def rest(j):
            i = 2 * j
            e_0, e_1, e_2, e_3 = e0[i], e0[i + 1], e0[i + 2], e0[i + 3]
            middle = e_1 + e_2
            total = around(e_0 + middle + (middle + e_3)) - middle
            rest0[j] = 0.4 * (wide[i + 1] + wide[i + 2]) + total

        loop(10, 10, rest)
        right = restrict_fine()
        g1[...] = right
        first = inv1[...] * right
        e1[...] = first
        total = first[1:7] + first[2:8] + first[3:9]
        remainder = 0.4 * right[2:8] + around(total) - first[2:8]
        return restrict_mid(remainder)

    def solve_coarsest(right):
        inverse = inv2[...]
        edge = jnp.zeros((1, 16, BZ), F32)
        e = inverse * right
        for _ in range(3):
            padded = jnp.concatenate([edge, e, edge], axis=0)
            total = around(padded[:-2] + padded[1:-1] + padded[2:])
            e = 0.4 * e + inverse * (right + total - e)
        coarse[pl.ds(1, CX * nx)] = e

    def up(keep):
        near = coarse[pl.ds(CX * gx, CX + 2)][:, :8]
        p_mid[:, pl.ds(0, 8, stride=2)] = near
        p_mid[:, pl.ds(1, 8, stride=2)] = near
        rise = select_dot(p_mid[...].reshape(5 * 16, BZ), m_p1[...]).reshape(5, 1, 16, BZ)
        rise = jnp.broadcast_to(rise, (5, 2, 16, BZ)).reshape(10, 16, BZ)
        e = e1[...] + rise
        total = around(e[0:8] + e[1:9] + e[2:10])
        e = 0.4 * e[1:9] + inv1[1:9] * (g1[1:9] + total - e[1:9])
        p_fine[:, pl.ds(0, 16, stride=2)] = e
        p_fine[:, pl.ds(1, 16, stride=2)] = e
        rest0[pl.ds(0, 8)] = select_dot(p_fine[...].reshape(8 * LY, BZ), m_p0[...]).reshape(8, LY, 2 * BZ)

        def add(j):
            i = 2 * j + 3
            e0[i] = e0[i] + rest0[j]
            e0[i + 1] = e0[i + 1] + rest0[j]

        loop(8, 8, add)

        def smooth(k):
            i = k + 4
            e = e0[i]
            total = around(e0[i - 1] + e + e0[i + 1])
            keep(i, 0.4 * e + inv0[i] * (wide[i] + total - e))

        loop(14, 14, smooth)

    def operate(keep):
        def body(x):
            i = x + HX
            value = wide[i]
            total = around(wide[i - 1] + value + wide[i + 1])
            value, total = value[8:24, :BZ], total[8:24, :BZ]
            keep(x, value, (27.0 + own[1, x]) * value - total)

        loop(BX, 12, body)

    def keep_wide(i, plane):
        wide[i] = plane

    for load in loads:
        load.wait()
    pack(0)
    pack(1)
    pl.semaphore_wait(barrier, count)

    start(fine_copies(1))
    start(fine_copies(0))
    far = [(2, k) for k in (4, nz - 4) if nz > 8] + [(0, k) for k in range(1, nx)]
    for axis, k in far:
        pl.semaphore_signal(hello, inc=1, device_id=along(axis, k), device_id_type=MESH)
    finish(fine_copies(1))
    widen(1)
    coefficients()
    finish(fine_copies(0))
    widen(0)
    put_coarse(0, down())
    start(deep_copies(0))
    finish(deep_copies(0))
    if far:
        pl.semaphore_wait(hello, len(far))
    shape = (CX * nx, 16, BZ)
    row = iota(shape, 1)
    y = CY * gy + jnp.where(row < 10, row - 2, row - 18)
    z = CZ * gz + wrapped(iota(shape, 2), 128)
    inv2[...] = masked_inverse(coarse_field(1), None, y, z, 1)
    edge = jnp.zeros((16, BZ), F32)
    coarse[0] = edge
    coarse[CX * nx + 1] = edge
    solve_coarsest(coarse_field(0))
    up(keep_wide)

    sums[...] = jnp.zeros_like(sums)

    def first_image(x, value, image):
        p_out[x] = value
        image_out[x] = image
        own[2, x] = image
        sums[0] += own[0, x] * value
        sums[1] += image * value

    operate(first_image)
    gamma = jnp.sum(sums[0], axis=0, keepdims=True)
    delta = jnp.sum(sums[1], axis=0, keepdims=True)
    low = iota((1, BZ), 1) < 64
    gamma, delta = gamma + pltpu.roll(gamma, 64, 1), delta + pltpu.roll(delta, 64, 1)
    line_start(0, jnp.where(low, gamma, delta))
    start(copy for copy in fine_copies(2) if copy[1][2] == 0)
    pack(2)
    start(copy for copy in fine_copies(2) if copy[1][2] != 0)
    finish(fine_copies(2))
    widen(2)
    put_coarse(2, down())
    start(deep_copies(1))
    line_start(1, line_finish(0))
    finish(deep_copies(1))
    solve_coarsest(coarse_field(2))
    up(keep_wide)

    def second_image(x, value, image):
        mw_out[x] = value
        nw_out[x] = image

    operate(second_image)
    for field in range(3):
        sent(fine_copies(field))
    for part in range(2):
        sent(deep_copies(part))
    for phase in range(2):
        line_whole(phase).wait_send()
    total = line_finish(1)
    gamma = jnp.sum(jnp.where(low, total, 0.0), axis=1, keepdims=True)
    delta = jnp.sum(jnp.where(low, 0.0, total), axis=1, keepdims=True)
    alpha_out[...] = jnp.broadcast_to(gamma / delta, alpha_out.shape)


def call(sizes, right_side, coefficient):
    nx = sizes[0]
    block = jax.ShapeDtypeStruct((BX, BY, BZ), F32)
    vmem_spec = pl.BlockSpec(memory_space=pltpu.VMEM)
    vmem = pltpu.VMEM
    return pl.pallas_call(
        functools.partial(kernel, sizes),
        out_shape=[block] * 4 + [jax.ShapeDtypeStruct((1, BZ), F32)],
        in_specs=[pl.BlockSpec(memory_space=pltpu.HBM)] * 2,
        out_specs=[vmem_spec] * 5,
        scratch_shapes=[
            vmem((3, BX, BY, BZ), F32),
            vmem((3, LX, LY, BZ), F32),
            vmem((2, 3, BX, 1, BZ), F32),
            vmem((2, 3, 3, LX, 1, BZ), F32),
            vmem((CX, 2, 1, BZ), F32),
            vmem((3, 3, CX * nx, 2, 1, BZ), F32),
            vmem((CX, 1, BZ), F32),
            vmem((3, 3, CX * nx, 1, BZ), F32),
            vmem((LX, LY, 2 * BZ), F32),
            vmem((LX, LY, 2 * BZ), F32),
            vmem((LX, LY, 2 * BZ), F32),
            vmem((10, LY, 2 * BZ), F32),
            vmem((10, 16, BZ), F32),
            vmem((10, 16, BZ), F32),
            vmem((10, 16, BZ), F32),
            vmem((CX * nx, 16, BZ), F32),
            vmem((CX * nx + 2, 16, BZ), F32),
            vmem((10, LY, BZ), F32),
            vmem((CX, 16, BZ), F32),
            vmem((5, 16, BZ), F32),
            vmem((8, LY, BZ), F32),
            vmem((BZ, 2 * BZ), BF16),
            vmem((2 * BZ, BZ), BF16),
            vmem((2 * BZ, BZ), BF16),
            vmem((BZ, BZ), BF16),
            vmem((BZ, BZ), BF16),
            vmem((BZ, 2 * BZ), BF16),
            vmem((2, BY, BZ), F32),
            vmem((2, 1, BZ), F32),
            vmem((nx * sizes[1], 1, BZ), F32),
            vmem((sizes[2], 1, BZ), F32),
            pltpu.SemaphoreType.DMA((2,)),
            pltpu.SemaphoreType.DMA((3, len(FINE))),
            pltpu.SemaphoreType.DMA((3, len(FINE))),
            pltpu.SemaphoreType.DMA((2, len(DEEP))),
            pltpu.SemaphoreType.DMA((2, len(DEEP))),
            pltpu.SemaphoreType.DMA((2,)),
            pltpu.SemaphoreType.DMA((2,)),
            pltpu.SemaphoreType.REGULAR,
        ],
        compiler_params=pltpu.CompilerParams(
            collective_id=0, has_side_effects=True, vmem_limit_bytes=16 * 1024 * 1024
        ),
    )(right_side, coefficient)


def solution(mesh):
    sizes = tuple(mesh.shape[axis] for axis in ("gx", "gy", "gz"))

    def shards(right_side, coefficient):
        held = [pltpu.with_memory_space_constraint(a, pltpu.HBM) for a in (right_side, coefficient)]
        precond, image, mw, nw, alpha = call(sizes, *held)
        alpha = alpha[None]
        return (
            alpha * precond,
            right_side - alpha * image,
            precond - alpha * mw,
            image - alpha * nw,
        )

    spec = P("gx", "gy", "gz")
    return jax.shard_map(
        shards, mesh=mesh, in_specs=(spec, spec), out_specs=(spec,) * 4, check_vma=False
    )
```
